32 devices in a mesh: grp: 1, exp: 32 (over z, y, x, core).
Axes of the slice: x: 2, y: 2, z: 4, core: 2. Of those that a mesh axis runs over, the one named last changes fastest.
Arguments:
- tokens: bfloat16 [512, 2048], P(('grp', 'exp')), may hold values from -6 to 6
- routed_expert_index: int32 [512, 6], P(('grp', 'exp')), may hold values from 0 to 15, all different within a row; in each aligned block of 16 rows (0 to 15, 16 to 31, ...) at most 8 rows name the same one
- routing_gate_weight: float32 [512, 6], P(('grp', 'exp')), may hold values from 0.05 to 0.5
- token_adapter_index: int32 [512], P('grp'), may hold values from 0 to 511
- gate_weight_pieces: bfloat16 [32, 2048, 704], P('exp'), may hold values from -0.125 to 0.125
- up_weight: bfloat16 [32, 2048, 704], P('exp'), may hold values from -0.125 to 0.125
- down_weight: bfloat16 [32, 704, 2048], P('exp'), may hold values from -0.15625 to 0.15625
- adapter_down_matrix: bfloat16 [2048, 8192], P('exp'), may hold values from -0.125 to 0.125
- adapter_up_matrix: bfloat16 [2048, 8192], P('exp'), may hold values from -1.5 to 1.5
Outputs:
- mixed: bfloat16 [512, 2048], P(('grp', 'exp'))
The draws below stay inside these ranges and needn't reach their ends.
Inputs may be any that keep to these rules, and one draw needn't show every extreme that they name: `routed_expert_index`: each token names 6 different experts; among the 16 tokens of one index of exp (aligned blocks of rows) no expert is named more than 8 times.
All inputs are finite; a program needn't handle non-finite values.
Results may differ from the reference program's by a relative error of at most 0.009.
Values may be sent and summed in bfloat16 or wider, within the bound.
A program may use at most 128 MiB of HBM per device.

```python
import math
import jax
import jax.numpy as jnp
import numpy as np
from jax import lax

MODEL_DIM = 2048
FF = 1408
TOP = 6
ADAPTER_RANK = 16
ADAPTER_COUNT = 512
TOKENS_PER_SHARD = 16
EXPERTS = 16
TOKENS = 512
CAP = 8
N_EXP = 32


def plant(entries, key, smallest, largest):
    index_at = [jax.random.randint(jax.random.fold_in(key, axis), (), 0, length) for axis, length in enumerate(entries.shape)]
    main_axis = entries.shape.index(max(entries.shape))
    next_to = index_at[:main_axis] + [(index_at[main_axis] + 1) % entries.shape[main_axis]] + index_at[main_axis + 1:]
    return entries.at[tuple(index_at)].set(smallest).at[tuple(next_to)].set(largest)


def block_levels(own_key, dims, cuts, least, largest):
    def one(axis_at, parts):
        heights = jax.random.uniform(jax.random.fold_in(jax.random.fold_in(own_key, 6), axis_at), (parts,), jnp.float32, least / len(cuts), largest / len(cuts))
        return jnp.repeat(jnp.exp(heights), dims[axis_at] // parts).reshape((-1,) + (1,) * (len(dims) - axis_at - 1))

    factor_of = one(*cuts[0])
    for cut in cuts[1:]:
        factor_of = factor_of * one(*cut)
    return factor_of


def rank_bounds(number_of, slope):
    weights = [(1 << 20) // math.isqrt(grade ** slope) + 1 for grade in range(1, number_of + 1)]
    scale = 1 + sum(weights) // (1 << 30)
    return np.cumsum(np.array([max(1, weight // scale) for weight in weights]))


def skewed_ids(stream_key, extent, number_of, lean):
    listing = rank_bounds(number_of, lean)
    ticket = jax.random.randint(jax.random.fold_in(stream_key, 1), extent, 0, int(listing[number_of - 1]))
    standing = jnp.searchsorted(jnp.asarray(listing, jnp.int32), ticket, side="right")
    return jax.random.permutation(jax.random.fold_in(stream_key, 2), number_of)[standing].astype(jnp.int32)


def assign_block(rng, own, number, rows, number_of, top, most, skew):
    order = jax.random.permutation(rng, number_of)
    heavy_load, ordinary = shares(number_of, rows * top, most, skew, True), shares(number_of, rows * top, most, skew, False)
    places = jnp.arange(number_of)

    def named(tallies, turn):
        used = int((tallies > 0).sum())
        fixed = max(1, used // 4)
        passed = fixed + (places - fixed + turn * (used - fixed)) % max(1, number_of - fixed)
        return jnp.zeros((number_of,), jnp.int32).at[order[jnp.where(places < fixed, places, passed)]].set(jnp.asarray(tallies, jnp.int32))

    tallies = jnp.where(number % 4 == 0, named(heavy_load, number // 4), named(ordinary, number - number // 4 - 1))
    mixed = jax.random.permutation(jax.random.fold_in(own, 3), number_of)
    donor, sink = mixed[0:number_of // 2 * 2:2], mixed[1:number_of // 2 * 2:2]
    room = jnp.minimum(tallies[donor] - 1, most - tallies[sink]) // 2
    room = jnp.where((donor == order[0]) | (sink == order[0]) | (tallies[sink] == 0), 0, jnp.maximum(room, 0))
    passed = jax.random.randint(jax.random.fold_in(own, 4), (number_of // 2,), 0, 1 << 20) % (room + 1)
    tallies = tallies.at[donor].add(-passed).at[sink].add(passed)
    members = jnp.searchsorted(jnp.cumsum(tallies), jnp.arange(rows * top), side="right").astype(jnp.int32)
    table = members.reshape(top, rows).T
    table = table[jax.random.permutation(jax.random.fold_in(own, 1), rows)]
    turn = jax.random.randint(jax.random.fold_in(own, 2), (rows, 1), 0, top)
    return jnp.take_along_axis(table, (jnp.arange(top)[None, :] + turn) % top, axis=1)


def shares(count, total, limit, skew, full):
    loads = [(1 << 20) // math.isqrt(rank ** skew) + 1 for rank in range(1, count + 1)]
    largest = limit if full else min(limit, max(-(-total // count), total * loads[0] // sum(loads)))
    least = 1 if total - largest >= count - 1 else 0
    counts, rest = [largest] + [least] * (count - 1), total - largest - least * (count - 1)
    while rest > 0:
        free = [i for i in range(1, count) if counts[i] < largest] or [i for i in range(1, count) if counts[i] < limit]
        whole, left = sum([loads[i] for i in free]), rest
        for i in free:
            more = min(limit - counts[i], max(1, left * loads[i] // whole), rest)
            counts[i] = counts[i] + more
            rest = rest - more
    return np.array(counts)


def gaussian(stream_key, extent, width, limit, shards=(), kind=jnp.bfloat16):
    drawn = jax.random.normal(stream_key, extent, jnp.float32) * width
    if len(shards) > 0:
        drawn = block_levels(stream_key, extent, shards, -0.22, 0.18) * drawn
    return jnp.clip(drawn, min=-limit, max=limit).astype(kind)


def setup_inputs(seed: int = 0, part: int = 0) -> dict:
    splits = jax.random.split(jax.random.key(seed), 10)
    part_keys = jax.random.split(jax.random.fold_in(splits[9], part), 10)
    tokens = gaussian(part_keys[0], (TOKENS, MODEL_DIM), 1.0, 6.0, ((0, 32),))
    routed_expert_index_keys = jax.random.split(jax.random.fold_in(part_keys[1], 1), TOKENS // TOKENS_PER_SHARD)
    routed_expert_index_turns = jax.random.permutation(jax.random.fold_in(part_keys[1], 3), TOKENS // TOKENS_PER_SHARD)
    routed_expert_index = jax.vmap(lambda own, number: assign_block(jax.random.fold_in(part_keys[1], 2), own, number, TOKENS_PER_SHARD, EXPERTS, TOP, CAP, 2))(routed_expert_index_keys, routed_expert_index_turns).reshape((TOKENS, TOP))
    routing_gate_weight = jnp.clip(jnp.exp(math.log(0.5) - 2.3025851 * jax.random.uniform(part_keys[2], (TOKENS, TOP), jnp.float32) ** block_levels(part_keys[2], (TOKENS, TOP), ((0, 32),), -0.2, 0.2)), 0.05, 0.5)
    token_adapter_index = plant(skewed_ids(part_keys[3], (TOKENS,), ADAPTER_COUNT, 2), jax.random.fold_in(part_keys[3], 3), 0, ADAPTER_COUNT - 1).astype(jnp.int32)
    gate_weight_pieces = gaussian(splits[4], (2 * EXPERTS, MODEL_DIM, FF // 2), MODEL_DIM ** -0.5, 0.125, ((0, 32),))
    up_weight = gaussian(splits[5], (2 * EXPERTS, MODEL_DIM, FF // 2), MODEL_DIM ** -0.5, 0.125, ((0, 32),))
    down_weight = gaussian(splits[6], (2 * EXPERTS, FF // 2, MODEL_DIM), FF ** -0.5, 0.15625, ((0, 32),))
    adapter_down_matrix = gaussian(splits[7], (MODEL_DIM, ADAPTER_COUNT * ADAPTER_RANK), MODEL_DIM ** -0.5, 0.125, ((0, 32),))
    adapter_up_matrix = gaussian(splits[8], (MODEL_DIM, ADAPTER_COUNT * ADAPTER_RANK), ADAPTER_RANK ** -0.5, 1.5, ((0, 32),))
    return dict(tokens=tokens, routed_expert_index=routed_expert_index, routing_gate_weight=routing_gate_weight, token_adapter_index=token_adapter_index, gate_weight_pieces=gate_weight_pieces, up_weight=up_weight, down_weight=down_weight, adapter_down_matrix=adapter_down_matrix, adapter_up_matrix=adapter_up_matrix)


def reference(tokens, routed_expert_index, routing_gate_weight, token_adapter_index, gate_weight_pieces, up_weight, down_weight, adapter_down_matrix, adapter_up_matrix):
    flat_ids = routed_expert_index.reshape(N_EXP, TOKENS_PER_SHARD * TOP)
    one_hot = (flat_ids[:, :, None] == jnp.arange(EXPERTS, dtype=jnp.int32)[None, None, :]).astype(jnp.int32)
    counted = jnp.cumsum(one_hot, axis=1)
    position = jnp.sum(one_hot * counted, axis=2) - 1
    block_ids = jnp.arange(N_EXP, dtype=jnp.int32)[:, None]
    column = (block_ids * CAP + position).reshape(-1).astype(jnp.int32)
    expert_col = flat_ids.reshape(-1).astype(jnp.int32)
    token_col = (jnp.arange(TOKENS * TOP, dtype=jnp.int32) // TOP).astype(jnp.int32)
    row_table = jnp.full((EXPERTS, N_EXP * CAP), TOKENS, jnp.int32).at[expert_col, column].set(token_col)
    row_gates = jnp.zeros((EXPERTS, N_EXP * CAP), jnp.float32).at[expert_col, column].set(routing_gate_weight.reshape(-1))
    padded = jnp.concatenate([tokens, jnp.zeros((1, MODEL_DIM), tokens.dtype)], axis=0)

    def one_expert(summed, expert):
        rows_index = row_table[expert]
        row_block = padded[rows_index]
        output = jnp.zeros((row_block.shape[0], MODEL_DIM), jnp.float32)
        for which in range(2):
            slab_index = 2 * expert + which
            gate_act = jnp.dot(row_block, gate_weight_pieces[slab_index], preferred_element_type=jnp.float32)
            up_act = jnp.dot(row_block, up_weight[slab_index], preferred_element_type=jnp.float32)
            hidden = (jax.nn.silu(gate_act) * up_act).astype(jnp.bfloat16)
            output = output + jnp.dot(hidden, down_weight[slab_index], preferred_element_type=jnp.float32)
        summed = summed.at[rows_index].add(row_gates[expert][:, None] * output)
        return summed, None

    start = jnp.zeros((TOKENS + 1, MODEL_DIM), jnp.float32)
    routed, _ = lax.scan(one_expert, start, jnp.arange(EXPERTS, dtype=jnp.int32))
    routed = routed[:TOKENS]

    down_adapter_matrix = adapter_down_matrix.reshape(MODEL_DIM, ADAPTER_COUNT, ADAPTER_RANK)
    up_adapter_matrix = adapter_up_matrix.reshape(MODEL_DIM, ADAPTER_COUNT, ADAPTER_RANK)

    def adapter_block_rows(input_rows):
        x_block, id_block = input_rows
        down_selected = down_adapter_matrix[:, id_block, :].astype(jnp.float32)
        low_rank = jnp.einsum("td,dtr->tr", x_block.astype(jnp.float32), down_selected).astype(jnp.bfloat16)
        up_selected = up_adapter_matrix[:, id_block, :].astype(jnp.float32)
        return jnp.einsum("tr,dtr->td", low_rank.astype(jnp.float32), up_selected).astype(jnp.bfloat16)

    lowrank_delta = lax.map(adapter_block_rows, (tokens.reshape(N_EXP, TOKENS_PER_SHARD, MODEL_DIM), token_adapter_index.reshape(N_EXP, TOKENS_PER_SHARD)))
    lowrank_delta = lowrank_delta.reshape(TOKENS, MODEL_DIM)
    return (routed + lowrank_delta.astype(jnp.float32)).astype(jnp.bfloat16)
```

```python
import functools

import jax
import jax.numpy as jnp
from jax import lax
from jax.experimental import pallas as pl
from jax.experimental.pallas import tpu as pltpu
from jax.sharding import PartitionSpec as P

RANK = 16
LANES = 128
BF16 = jnp.bfloat16
F32 = jnp.float32
MESH = pl.DeviceIdType.MESH


def dot_nt(a, b):
    return lax.dot_general(a, b, (((1,), (1,)), ((), ())), preferred_element_type=F32)


def kernel(
    line, plane, cap, top, x_ref, idx_ref, gate_ref, aid_ref, wg_hbm, wu_hbm, wd_hbm, adn_hbm, aup_hbm, out_ref,
    wg, wu, wd, adn, aup, line_x, comb_send, line_comb, col, disp, recv_a, recv_b, xs, hid, y_own, sib_send, sib_recv,
    lr_send, lr1_recv, lr2_send, lr2_recv, cor_send, cor_recv, ret_send, ret_recv, part_send, part_recv, own_part,
    w_sem, adl_sem, ad_s, ad_r, x_s, x_r, cb_s, cb_r, col_s, col_r, disp_s, disp_r, fwd_s, fwd_r, l1_s, l1_r,
    l2_s, l2_r, cor_s, cor_r, ret_s, ret_r, part_s, part_r, sib_s, sib_r,
):
    me = lax.axis_index("exp")
    q = lax.div(me, 2)
    c = lax.rem(me, 2)
    z = lax.div(q, plane)
    g = lax.rem(q, plane)
    sib = me + 1 - 2 * c
    rows, width = x_ref.shape
    feats = adn_hbm.shape[0]
    bank = adn_hbm.shape[1]
    chips = line * plane
    group = chips * rows
    slots = chips * cap
    block = plane * cap
    wide_n = width // line
    off = pl.multiple_of(lax.rem(me * feats, LANES), feats)
    half_l = LANES // 2

    def remote(src, dst, ss, rs, dev):
        return pltpu.make_async_remote_copy(
            src_ref=src, dst_ref=dst, send_sem=ss, recv_sem=rs, device_id={"exp": dev}, device_id_type=MESH
        )

    def dev_z(to):
        return 2 * (to * plane + g) + c

    def dev_g(to):
        return 2 * (z * plane + to) + c

    side = lax.div(2 * z, line)
    mirror = side * z + (1 - side) * (line - 1 - z)

    def far(s):
        d = s + lax.div(s - mirror + line, line)
        return side * d + (1 - side) * (line - 1 - d)

    def loop(n, fn):
        def step(r, carry):
            fn(r)
            return carry

        lax.fori_loop(0, n, step, 0)

    def line_far(fn):
        loop(line - 1, lambda s: fn(far(s)))

    def line_near(fn):
        loop(line - 1, lambda s: fn(far(line - 2 - s)))

    def plane_peers(fn):
        loop(plane - 1, lambda r: fn(lax.rem(g + 1 + r, plane)))

    barrier = pltpu.get_barrier_semaphore()
    if 2 * feats < LANES:
        adn[...] = jnp.zeros_like(adn)
        aup[...] = jnp.zeros_like(aup)

    def greet(dev):
        pl.semaphore_signal(barrier, inc=1, device_id={"exp": dev}, device_id_type=MESH)

    line_far(lambda d: greet(dev_z(d)))
    plane_peers(lambda d: greet(dev_g(d)))
    greet(sib)

    own_rows = pl.ds(off, feats)
    local = [
        pltpu.make_async_copy(adn_hbm, adn.at[own_rows], adl_sem.at[0]),
        pltpu.make_async_copy(wg_hbm.at[0], wg, w_sem.at[0]),
        pltpu.make_async_copy(wu_hbm.at[0], wu, w_sem.at[1]),
        pltpu.make_async_copy(aup_hbm, aup.at[own_rows], adl_sem.at[1]),
        pltpu.make_async_copy(wd_hbm.at[0], wd, w_sem.at[2]),
    ]
    for cp in local:
        cp.start()

    slot = lax.broadcasted_iota(jnp.int32, (slots, rows), 0)
    slot_e = lax.div(slot, cap)
    chosen = jnp.zeros((slots, rows), F32)
    weight = jnp.zeros((slots, rows), F32)
    for k in range(top):
        hit = idx_ref[k : k + 1, :] == slot_e
        chosen = chosen + jnp.where(hit, 1.0, 0.0)
        weight = weight + jnp.where(hit, gate_ref[k : k + 1, :], 0.0)
    earlier = jnp.where(
        lax.broadcasted_iota(jnp.int32, (rows, rows), 0) < lax.broadcasted_iota(jnp.int32, (rows, rows), 1), 1.0, 0.0
    )
    rank_of = jnp.dot(chosen.astype(BF16), earlier.astype(BF16), preferred_element_type=F32)
    slot_p = lax.rem(slot, cap).astype(F32)
    combine = jnp.where((chosen > 0.5) & (rank_of == slot_p), weight, 0.0)
    for d in range(line):
        part = combine[d * block : (d + 1) * block].T
        hi = part.astype(BF16)
        lo = (part - hi.astype(F32)).astype(BF16)
        comb_send[d, :, :block] = hi
        comb_send[d, :, half_l : half_l + block] = lo
    line_comb[pl.ds(z, 1)] = comb_send[pl.ds(z, 1)]
    line_x[pl.ds(z, 1)] = x_ref[...].reshape(1, rows, width)

    pl.semaphore_wait(barrier, line + plane - 1)

    def lanes_of(chip):
        return pl.ds(pl.multiple_of(lax.div(chip * 2 * feats, LANES) * LANES, LANES), LANES)

    def chunk_of(i):
        return pl.ds(pl.multiple_of(i * wide_n, wide_n), wide_n)

    def x_copy(to, slot, i):
        return remote(
            x_ref.at[:, chunk_of(i)], line_x.at[slot, :, chunk_of(i)],
            x_s.at[to * line + i], x_r.at[slot * line + i], dev_z(to),
        )

    def comb_copy(to, slot):
        return remote(comb_send.at[to], line_comb.at[slot], cb_s.at[to], cb_r.at[slot], dev_z(to))

    def col_copy(to, slot, s):
        return remote(
            line_x.at[s, :, lanes_of(z * plane + to)], col.at[slot, s],
            col_s.at[to * line + s], col_r.at[slot * line + s], dev_g(to),
        )

    def disp_copy(to, slot, s):
        return remote(
            disp.at[to, s], recv_a.at[slot, s], disp_s.at[to * line + s], disp_r.at[slot * line + s], dev_g(to)
        )

    def fwd_copy(slot, s):
        at = slot * line + s
        return remote(recv_a.at[slot, s], recv_b.at[slot, s], fwd_s.at[at], fwd_r.at[at], sib)

    def lr1_copy(to, slot):
        return remote(lr_send, lr1_recv.at[slot], l1_s.at[to], l1_r.at[slot], dev_g(to))

    def lr2_copy(to, slot):
        return remote(lr2_send, lr2_recv.at[slot], l2_s.at[to], l2_r.at[slot], dev_z(to))

    def cor_copy(to, slot):
        return remote(cor_send.at[to], cor_recv.at[slot], cor_s.at[to], cor_r.at[slot], dev_g(to))

    def ret_copy(i, to, slot):
        return remote(
            ret_send.at[i, to], ret_recv.at[i, slot], ret_s.at[i * plane + to], ret_r.at[i * plane + slot], dev_g(to)
        )

    def turn_of(i, at):
        return lax.rem(at + 1 + i, line)

    def part_copy(i, to, slot, j):
        return remote(
            part_send.at[i, to], part_recv.at[slot, j], part_s.at[i * line + to], part_r.at[slot * line + j], dev_z(to)
        )

    def sib_copy(i):
        return remote(sib_send.at[i], sib_recv.at[i], sib_s.at[i], sib_r.at[i], sib)

    def send_x(i):
        line_far(lambda d: x_copy(d, z, lax.rem(d + i, line)).start())

    def own_col(s):
        col[pl.ds(g, 1), pl.ds(s, 1)] = line_x[pl.ds(s, 1), :, lanes_of(q)].reshape(1, 1, rows, LANES)

    send_x(0)
    plane_peers(lambda d: col_copy(d, g, z).start())
    line_far(lambda d: comb_copy(d, z).start())
    for i in range(1, line):
        send_x(i)
    adn_copy = remote(adn_hbm, adn.at[own_rows], ad_s.at[0], ad_r.at[0], sib)
    aup_copy = remote(aup_hbm, aup.at[own_rows], ad_s.at[1], ad_r.at[1], sib)
    adn_copy.start()

    def pack(s):
        pick = jnp.where(line_comb[s].astype(F32) > 0.0, 1.0, 0.0).T[:block].astype(BF16)
        packed = jnp.dot(pick, line_x[s], preferred_element_type=F32)
        disp[:, pl.ds(s, 1)] = packed.reshape(plane, 1, cap, width).astype(BF16)
        recv_a[pl.ds(g, 1), pl.ds(s, 1)] = disp[pl.ds(g, 1), pl.ds(s, 1)]
        plane_peers(lambda d: disp_copy(d, g, s).start())
        fwd_copy(g, s).start()

    pack(z)
    aup_copy.start()
    own_col(z)

    per = LANES // RANK
    ids = []
    near = line * rows
    for p in range(plane):
        lane = lax.broadcasted_iota(jnp.int32, (near, aid_ref.shape[1]), 1)
        row = lax.broadcasted_iota(jnp.int32, (near, aid_ref.shape[1]), 0)
        here = ((lax.div(row, rows) * plane + p) * 2 + c) * rows + lax.rem(row, rows)
        ids.append(jnp.sum(jnp.where(lane == here, aid_ref[...].astype(F32), 0.0), axis=1, keepdims=True))
    ids = jnp.broadcast_to(jnp.concatenate(ids, axis=0), (group, LANES)).astype(jnp.int32)
    id_hi = lax.div(ids, per)
    id_lo = ids - id_hi * per
    lane_g = lax.broadcasted_iota(jnp.int32, (group, LANES), 1)
    keep = lax.div(lane_g, RANK) == id_lo

    def relay_cols(s):
        x_copy(z, s, z).wait_recv()
        plane_peers(lambda d: col_copy(d, g, s).start())
        own_col(s)

    def relay_x(s):
        for i in range(1, line):
            x_copy(z, s, lax.rem(z + i, line)).wait_recv()
        comb_copy(z, s).wait_recv()
        pack(s)

    line_near(relay_cols)
    line_near(relay_x)

    plane_peers(lambda p: loop(line, lambda s: col_copy(g, p, s).wait_recv()))
    local[0].wait()
    adn_copy.wait_recv()
    cols = col[...].reshape(group, LANES)
    span = 512
    sub = span // LANES

    def down_step(i, acc):
        at = pl.multiple_of(i * span, span)
        h = jnp.dot(cols, adn[:, pl.ds(at, span)], preferred_element_type=F32)
        for s in range(sub):
            acc = jnp.where(id_hi == i * sub + s, h[:, s * LANES : (s + 1) * LANES], acc)
        return acc

    terms = lax.fori_loop(0, bank // span, down_step, jnp.zeros((group, LANES), F32))
    terms = jnp.where(keep, terms, 0.0).astype(BF16)
    fi = lax.broadcasted_iota(jnp.int32, (LANES, LANES), 0)
    fj = lax.broadcasted_iota(jnp.int32, (LANES, LANES), 1)
    fold = jnp.where(lax.rem(fi, RANK) == lax.rem(fj, RANK), 1.0, 0.0).astype(BF16)
    turn = lax.div(lane_g, RANK) == lax.rem(lax.broadcasted_iota(jnp.int32, (group, LANES), 0), per)
    folded = jnp.where(turn, jnp.dot(terms, fold, preferred_element_type=F32), 0.0)
    lr_send[...] = jnp.sum(folded.reshape(group // per, per, LANES), axis=1)
    lr1_recv[pl.ds(g, 1)] = lr_send[...].reshape(1, group // per, LANES)
    plane_peers(lambda d: lr1_copy(d, g).start())

    def forward(s):
        def one(p):
            disp_copy(g, p, s).wait_recv()
            fwd_copy(p, s).start()

        plane_peers(one)

    forward(z)
    plane_peers(lambda p: lr1_copy(g, p).wait_recv())
    lr2_send[...] = jnp.sum(lr1_recv[...], axis=0)
    lr2_recv[pl.ds(z, 1)] = lr2_send[...].reshape(1, group // per, LANES)
    line_far(lambda d: lr2_copy(d, z).start())
    line_near(forward)

    half = wd.shape[0]
    xs[:slots] = recv_a[...].astype(F32).reshape(slots, width).astype(BF16)
    local[1].wait()
    local[2].wait()
    local[4].wait()
    loop(plane, lambda p: loop(line, lambda s: fwd_copy(p, s).wait_recv()))
    xs[slots:] = recv_b[...].astype(F32).reshape(slots, width).astype(BF16)
    cut = -(-half // (2 * LANES)) * LANES
    for a, b in ((0, cut), (cut, half)):
        gt = dot_nt(wg[a:b], xs[...])
        up = dot_nt(wu[a:b], xs[...])
        hid[:, a:b] = (gt / (1.0 + jnp.exp(-gt)) * up).T.astype(BF16)

    def down_part(i):
        y = jnp.dot(hid[...], wd[:, chunk_of(turn_of(i, z))], preferred_element_type=F32)
        sib_send[i] = y[slots:].reshape(plane, line, cap, wide_n).astype(BF16)
        sib_copy(i).start()
        y_own[i] = y[:slots]

    def finish(i):
        sib_copy(i).wait_recv()
        ret_send[i] = (y_own[i].reshape(plane, line, cap, wide_n) + sib_recv[i].astype(F32)).astype(BF16)
        ret_recv[i, pl.ds(g, 1)] = ret_send[i, pl.ds(g, 1)]
        plane_peers(lambda d: ret_copy(i, d, g).start())

    for i in range(line):
        down_part(i)
        if i > 0:
            finish(i - 1)
    finish(line - 1)

    line_near(lambda s: lr2_copy(z, s).wait_recv())
    local[3].wait()
    aup_copy.wait_recv()
    low = jnp.sum(lr2_recv[...], axis=0).astype(BF16).astype(F32)
    ranks = jnp.broadcast_to(low.reshape(group // per, 1, LANES), (group // per, per, LANES)).reshape(group, LANES)
    ranks = jnp.where(turn, ranks, 0.0).astype(BF16)
    ranks = jnp.where(keep, jnp.dot(ranks, fold, preferred_element_type=F32), 0.0)

    def up_step(i, acc):
        at = pl.multiple_of(i * span, span)
        wide = jnp.concatenate([jnp.where(id_hi == i * sub + s, ranks, 0.0).astype(BF16) for s in range(sub)], axis=1)
        return acc + dot_nt(wide, aup[:, pl.ds(at, span)])

    corr = lax.fori_loop(0, bank // span, up_step, jnp.zeros((group, LANES), F32))
    cor_send[...] = corr.astype(BF16).reshape(plane, line, rows, LANES)
    cor_recv[pl.ds(g, 1)] = cor_send[pl.ds(g, 1)]
    plane_peers(lambda d: cor_copy(d, g).start())

    share = LANES // (2 * feats)

    def mix(i):
        plane_peers(lambda p: ret_copy(i, g, p).wait_recv())
        j = turn_of(i, z)
        if i == line - 1:
            plane_peers(lambda p: cor_copy(g, p).wait_recv())
        for s in range(line):
            back = ret_recv[i, :, s].astype(F32).reshape(block, wide_n).astype(BF16)
            both = line_comb[s]
            routed = jnp.dot(both[:, :block], back, preferred_element_type=F32)
            routed = routed + jnp.dot(both[:, half_l : half_l + block], back, preferred_element_type=F32)
            if i == line - 1:
                delta = []
                for b in range(wide_n // LANES):
                    one = cor_recv[b * share, s].astype(F32)
                    for t in range(1, share):
                        one = one + cor_recv[b * share + t, s].astype(F32)
                    delta.append(one)
                routed = routed + jnp.concatenate(delta, axis=1)
            part_send[i, s] = routed.astype(BF16)
        own_part[pl.ds(j, 1)] = part_send[i, pl.ds(z, 1)].astype(F32)
        line_far(lambda d: part_copy(i, d, z, j).start())

    for i in range(line):
        mix(i)

    for i in range(line):
        line_near(lambda s: part_copy(i, z, s, turn_of(i, s)).wait_recv())
    for j in range(line):
        def add(s, acc):
            return acc + part_recv[far(s), j].astype(F32)

        out_ref[:, j * wide_n : (j + 1) * wide_n] = lax.fori_loop(0, line - 1, add, own_part[j]).astype(BF16)

    adn_copy.wait_send()
    aup_copy.wait_send()
    for i in range(line):
        sib_copy(i).wait_send()

    def drain_line(d):
        comb_copy(d, z).wait_send()
        lr2_copy(d, z).wait_send()
        for i in range(line):
            x_copy(d, z, i).wait_send()
            part_copy(i, d, z, i).wait_send()

    def drain_plane(d):
        lr1_copy(d, g).wait_send()
        cor_copy(d, g).wait_send()
        loop(line, lambda s: col_copy(d, g, s).wait_send())
        loop(line, lambda s: disp_copy(d, g, s).wait_send())
        for i in range(line):
            ret_copy(i, d, g).wait_send()

    line_far(drain_line)
    plane_peers(drain_plane)
    loop(plane, lambda p: loop(line, lambda s: fwd_copy(p, s).wait_send()))


def per_device(tokens, idx, gates, aid, wg, wu, wd, adn, aup):
    devices = lax.axis_size("exp")
    chips = devices // 2
    plane = 1
    while plane * plane < chips:
        plane *= 2
    line = chips // plane
    rows, width = tokens.shape
    top = idx.shape[1]
    half = wd.shape[1]
    feats, bank = adn.shape
    need = 2 * (rows * top // devices + 1)
    cap = -(-need // 8) * 8
    slots = chips * cap
    short = chips * rows * RANK // LANES
    wide_n = width // line
    blocks = lambda *s: pltpu.VMEM(s, BF16)
    full = lambda *s: pltpu.VMEM(s, F32)
    sems = lambda n: pltpu.SemaphoreType.DMA((n,))
    vm = pl.BlockSpec(memory_space=pltpu.VMEM)
    hbm = pl.BlockSpec(memory_space=pl.ANY)
    return pl.pallas_call(
        functools.partial(kernel, line, plane, cap, top),
        out_shape=jax.ShapeDtypeStruct((rows, width), BF16),
        in_specs=[vm, vm, vm, vm, hbm, hbm, hbm, hbm, hbm],
        out_specs=vm,
        scratch_shapes=[
            blocks(half, width), blocks(half, width), blocks(half, width),
            blocks(LANES, bank), blocks(LANES, bank),
            blocks(line, rows, width), blocks(line, rows, LANES), blocks(line, rows, LANES),
            blocks(plane, line, rows, LANES),
            blocks(plane, line, cap, width), blocks(plane, line, cap, width), blocks(plane, line, cap, width),
            blocks(2 * slots, width), blocks(2 * slots, half), full(line, slots, wide_n),
            blocks(line, plane, line, cap, wide_n), blocks(line, plane, line, cap, wide_n),
            full(short, LANES), full(plane, short, LANES), full(short, LANES), full(line, short, LANES),
            blocks(plane, line, rows, LANES), blocks(plane, line, rows, LANES),
            blocks(line, plane, line, cap, wide_n), blocks(line, plane, line, cap, wide_n),
            blocks(line, line, rows, wide_n), blocks(line, line, rows, wide_n), full(line, rows, wide_n),
            sems(3), sems(2), sems(2), sems(2),
            sems(line * line), sems(line * line), sems(line), sems(line),
            sems(plane * line), sems(plane * line), sems(plane * line), sems(plane * line),
            sems(plane * line), sems(plane * line),
            sems(plane), sems(plane), sems(line), sems(line), sems(plane), sems(plane),
            sems(line * plane), sems(line * plane), sems(line * line), sems(line * line), sems(line), sems(line),
        ],
        compiler_params=pltpu.CompilerParams(
            collective_id=0, has_side_effects=True, vmem_limit_bytes=60 * 1024 * 1024
        ),
    )(tokens, idx.T, gates.T, aid.reshape(1, -1), wg.swapaxes(1, 2), wu.swapaxes(1, 2), wd, adn, aup)


def solution(mesh):
    placed = (
        P(("grp", "exp"), None),
        P(("grp", "exp"), None),
        P(("grp", "exp"), None),
        P("grp"),
        P("exp", None, None),
        P("exp", None, None),
        P("exp", None, None),
        P("exp", None),
        P("exp", None),
    )
    return jax.shard_map(
        per_device, mesh=mesh, in_specs=placed, out_specs=P(("grp", "exp"), None), check_vma=False
    )
```

```python
import functools

import jax
import jax.numpy as jnp
from jax import lax
from jax.experimental import pallas as pl
from jax.experimental.pallas import tpu as pltpu
from jax.sharding import PartitionSpec as P

RANK = 16
LANES = 128
BF16 = jnp.bfloat16
F32 = jnp.float32
MESH = pl.DeviceIdType.MESH


def dot_nt(a, b):
    return lax.dot_general(a, b, (((1,), (1,)), ((), ())), preferred_element_type=F32)


def kernel(
    line, plane, cap, top, x_hbm, idx_hbm, gate_hbm, aid_hbm, wg_hbm, wu_hbm, wd_hbm, adn_hbm, aup_hbm, out_hbm,
    out_ref,    idx_ref, gate_ref, aid_ref, wg, wu, wd, adn, aup, line_x, comb_send, line_comb, pick_ref, col, disp, recv_a, recv_b, xs, gt_ref, up_ref, hid, y_own, sib_send, sib_recv,
    tag_ref, tag_t, keep_ref, lr_send, lr1_recv, lr2_send, lr2_recv, cor_send, cor_recv, ret_send, ret_recv, part_send, part_recv, own_part,
 in_sem, out_sem, w_sem, adl_sem, ad_s, ad_r, x_s, x_r, cb_s, cb_r, col_s, col_r, disp_s, disp_r, fwd_s, fwd_r, l1_s, l1_r,
    l2_s, l2_r, cor_s, cor_r, ret_s, ret_r, part_s, part_r, sib_s, sib_r,
):
    me = lax.axis_index("exp")
    q = lax.div(me, 2)
    c = lax.rem(me, 2)
    z = lax.div(q, plane)
    g = lax.rem(q, plane)
    sib = me + 1 - 2 * c
    rows, width = x_hbm.shape
    feats = adn_hbm.shape[0]
    bank = adn_hbm.shape[1]
    chips = line * plane
    group = chips * rows
    slots = chips * cap
    block = plane * cap
    wide_n = width // line
    off = pl.multiple_of(lax.rem(me * feats, LANES), feats)
    half_l = LANES // 2

    def remote(src, dst, ss, rs, dev):
        return pltpu.make_async_remote_copy(
            src_ref=src, dst_ref=dst, send_sem=ss, recv_sem=rs, device_id={"exp": dev}, device_id_type=MESH
        )

    def dev_z(to):
        return 2 * (to * plane + g) + c

    def dev_g(to):
        return 2 * (z * plane + to) + c

    side = lax.div(2 * z, line)
    mirror = side * z + (1 - side) * (line - 1 - z)

    def far(s):
        d = s + lax.div(s - mirror + line, line)
        return side * d + (1 - side) * (line - 1 - d)

    def loop(n, fn):
        def step(r, carry):
            fn(r)
            return carry

        lax.fori_loop(0, n, step, 0)

    def line_far(fn):
        loop(line - 1, lambda s: fn(far(s)))

    def line_near(fn):
        loop(line - 1, lambda s: fn(far(line - 2 - s)))

    def plane_peers(fn):
        loop(plane - 1, lambda r: fn(lax.rem(g + 1 + r, plane)))

    barrier = pltpu.get_barrier_semaphore()
    if 2 * feats < LANES:
        adn[...] = jnp.zeros_like(adn)
        aup[...] = jnp.zeros_like(aup)

    def greet(dev):
        pl.semaphore_signal(barrier, inc=1, device_id={"exp": dev}, device_id_type=MESH)

    line_far(lambda d: greet(dev_z(d)))
    plane_peers(lambda d: greet(dev_g(d)))
    greet(sib)

    own_rows = pl.ds(off, feats)
    inputs = [
        pltpu.make_async_copy(idx_hbm, idx_ref, in_sem.at[0]),
        pltpu.make_async_copy(gate_hbm, gate_ref, in_sem.at[1]),
        pltpu.make_async_copy(x_hbm, line_x.at[z], in_sem.at[2]),
        pltpu.make_async_copy(aid_hbm, aid_ref, in_sem.at[3]),
    ]
    for cp in inputs:
        cp.start()
    local = [
        pltpu.make_async_copy(adn_hbm, adn.at[own_rows], adl_sem.at[0]),
        pltpu.make_async_copy(wg_hbm.at[0], wg, w_sem.at[0]),
        pltpu.make_async_copy(wu_hbm.at[0], wu, w_sem.at[1]),
        pltpu.make_async_copy(aup_hbm, aup.at[own_rows], adl_sem.at[1]),
        pltpu.make_async_copy(wd_hbm.at[0], wd, w_sem.at[2]),
    ]
    for cp in inputs:
        cp.wait()
    for cp in local:
        cp.start()
    pl.semaphore_wait(barrier, line + plane - 1)

    def step_of(k, at):
        return at if k == 0 else k - 1 + lax.div(k - 1 + line - at, line)

    def lanes_of(chip):
        return pl.ds(pl.multiple_of(lax.div(chip * 2 * feats, LANES) * LANES, LANES), LANES)

    def chunk_of(i):
        return pl.ds(pl.multiple_of(i * wide_n, wide_n), wide_n)

    def x_copy(to, slot, i, kind):
        at = chunk_of(i)
        return remote(line_x.at[z, :, at], line_x.at[slot, :, at], x_s.at[0], x_r.at[kind * line + slot], dev_z(to))

    def comb_copy(to, slot):
        return remote(comb_send.at[to], line_comb.at[slot], cb_s.at[0], cb_r.at[slot], dev_z(to))

    def col_copy(to, slot, s):
        return remote(
            line_x.at[s, :, lanes_of(z * plane + to)], col.at[slot, s], col_s.at[0], col_r.at[0], dev_g(to)
        )

    def disp_copy(to, slot, s, k):
        at = chunk_of(step_of(k, z))
        return remote(disp.at[to, s, :, at], recv_a.at[slot, s, :, at], disp_s.at[0], disp_r.at[k], dev_g(to))

    def fwd_copy(k):
        at = chunk_of(step_of(k, z))
        return remote(recv_a.at[:, :, :, at], recv_b.at[:, :, :, at], fwd_s.at[k], fwd_r.at[k], sib)

    def lr1_copy(to, slot):
        return remote(lr_send, lr1_recv.at[slot], l1_s.at[0], l1_r.at[0], dev_g(to))

    def lr2_copy(to, slot):
        return remote(lr2_send, lr2_recv.at[slot], l2_s.at[0], l2_r.at[0], dev_z(to))

    def cor_copy(to, slot):
        return remote(cor_send.at[to], cor_recv.at[slot], cor_s.at[0], cor_r.at[0], dev_g(to))

    def ret_copy(i, to, slot):
        return remote(ret_send.at[i, to], ret_recv.at[i, slot], ret_s.at[0], ret_r.at[i], dev_g(to))

    def turn_of(i, at):
        return lax.rem(at + 1 + i, line)

    def part_copy(i, to, slot, j):
        return remote(part_send.at[i, to], part_recv.at[slot, j], part_s.at[0], part_r.at[0], dev_z(to))

    def sib_copy(i):
        return remote(sib_send.at[i], sib_recv.at[i], sib_s.at[i], sib_r.at[i], sib)

    rest_z = pl.ds(0, line - 1)
    rest_g = pl.ds(0, plane - 1)
    all_x = remote(line_x.at[rest_z], line_x.at[rest_z], x_s.at[0], x_r.at[0], sib)
    all_comb = remote(comb_send.at[rest_z], line_comb.at[rest_z], cb_s.at[0], cb_r.at[0], sib)
    all_col = remote(col.at[rest_g], col.at[rest_g], col_s.at[0], col_r.at[0], sib)
    all_disp = remote(disp.at[rest_g], recv_a.at[rest_g], disp_s.at[0], disp_r.at[0], sib)
    all_lr1 = remote(lr1_recv.at[rest_g], lr1_recv.at[rest_g], l1_s.at[0], l1_r.at[0], sib)
    all_lr2 = remote(lr2_recv.at[rest_z], lr2_recv.at[rest_z], l2_s.at[0], l2_r.at[0], sib)
    all_cor = remote(cor_send.at[rest_g], cor_recv.at[rest_g], cor_s.at[0], cor_r.at[0], sib)
    all_ret = remote(ret_send.at[:, rest_g], ret_recv.at[:, rest_g], ret_s.at[0], ret_r.at[0], sib)
    all_part = remote(part_send.at[:, rest_z], part_recv.at[rest_z], part_s.at[0], part_r.at[0], sib)

    def some_x(s, k):
        at = chunk_of(0)
        return remote(line_x.at[s, :, at], line_x.at[s, :, at], x_s.at[0], x_r.at[k * line + s], sib)

    def some_disp(k):
        at = chunk_of(0)
        return remote(disp.at[rest_g, :, :, at], recv_a.at[rest_g, :, :, at], disp_s.at[0], disp_r.at[k], sib)

    def some_ret(i):
        return remote(ret_send.at[i, rest_g], ret_recv.at[i, rest_g], ret_s.at[0], ret_r.at[i], sib)

    line_far(lambda d: x_copy(d, z, step_of(0, d), 0).start())
    plane_peers(lambda d: col_copy(d, g, z).start())
    slot = lax.broadcasted_iota(jnp.int32, (slots, rows), 0)
    slot_e = lax.div(slot, cap)
    chosen = jnp.zeros((slots, rows), F32)
    weight = jnp.zeros((slots, rows), F32)
    for k in range(top):
        hit = idx_ref[k : k + 1, :] == slot_e
        chosen = chosen + jnp.where(hit, 1.0, 0.0)
        weight = weight + jnp.where(hit, gate_ref[k : k + 1, :], 0.0)
    earlier = jnp.where(
        lax.broadcasted_iota(jnp.int32, (rows, rows), 0) < lax.broadcasted_iota(jnp.int32, (rows, rows), 1), 1.0, 0.0
    )
    rank_of = jnp.dot(chosen.astype(BF16), earlier.astype(BF16), preferred_element_type=F32)
    slot_p = lax.rem(slot, cap).astype(F32)
    combine = jnp.where((chosen > 0.5) & (rank_of == slot_p), weight, 0.0)
    for d in range(line):
        part = combine[d * block : (d + 1) * block].T
        hi = part.astype(BF16)
        lo = (part - hi.astype(F32)).astype(BF16)
        comb_send[d, :, :block] = hi
        comb_send[d, :, half_l : half_l + block] = lo
    line_comb[pl.ds(z, 1)] = comb_send[pl.ds(z, 1)]

    line_far(lambda d: comb_copy(d, z).start())
    for k in range(1, line):
        line_far(lambda d: x_copy(d, z, step_of(k, d), k).start())
    adn_copy = remote(adn_hbm, adn.at[own_rows], ad_s.at[0], ad_r.at[0], sib)
    aup_copy = remote(aup_hbm, aup.at[own_rows], ad_s.at[1], ad_r.at[1], sib)
    adn_copy.start()
    aup_copy.start()

    def own_col(s):
        col[pl.ds(g, 1), pl.ds(s, 1)] = line_x[pl.ds(s, 1), :, lanes_of(q)].reshape(1, 1, rows, LANES)

    def take_pick(s):
        pick = jnp.where(line_comb[s].astype(F32) > 0.0, 1.0, 0.0).T[:block]
        pick_ref[pl.ds(s, 1)] = pick.astype(BF16).reshape(1, block, rows)

    def pack(s, k):
        at = chunk_of(step_of(k, z))
        packed = jnp.dot(pick_ref[s], line_x[s, :, at], preferred_element_type=F32)
        disp[:, pl.ds(s, 1), :, at] = packed.reshape(plane, 1, cap, wide_n).astype(BF16)
        recv_a[pl.ds(g, 1), pl.ds(s, 1), :, at] = disp[pl.ds(g, 1), pl.ds(s, 1), :, at]
        plane_peers(lambda d: disp_copy(d, g, s, k).start())

    take_pick(z)
    for k in range(line):
        pack(z, k)
    own_col(z)

    near_z = [far(line - 2 - k) for k in range(line - 1)]
    half = wd.shape[0]
    cut = -(-half // (2 * LANES)) * LANES

    def relay(k):
        for s in near_z:
            some_x(s, k).wait_recv()
            if k == 0:
                plane_peers(lambda d: col_copy(d, g, s).start())
                own_col(s)
                comb_copy(z, s).wait_recv()
                take_pick(s)
            pack(s, k)

    def receive(k):
        at = chunk_of(step_of(k, z))
        some_disp(k).wait_recv()
        fwd_copy(k).start()
        xs[:slots, at] = recv_a[:, :, :, at].astype(F32).reshape(slots, wide_n).astype(BF16)

    def multiply(k):
        at = chunk_of(step_of(k, z))
        fwd_copy(k).wait_recv()
        xs[slots:, at] = recv_b[:, :, :, at].astype(F32).reshape(slots, wide_n).astype(BF16)
        if k == 0:
            local[1].wait()
            local[2].wait()
        for a, b in ((0, cut), (cut, half)):
            gt = dot_nt(wg[a:b, at], xs[:, at])
            up = dot_nt(wu[a:b, at], xs[:, at])
            if k > 0:
                gt = gt + gt_ref[a:b]
                up = up + up_ref[a:b]
            if k < line - 1:
                gt_ref[a:b] = gt
                up_ref[a:b] = up
            else:
                hid[:, a:b] = (gt / (1.0 + jnp.exp(-gt)) * up).T.astype(BF16)

    relay(0)
    per = LANES // RANK
    ids = []
    near = line * rows
    for p in range(plane):
        lane = lax.broadcasted_iota(jnp.int32, (near, aid_ref.shape[1]), 1)
        row = lax.broadcasted_iota(jnp.int32, (near, aid_ref.shape[1]), 0)
        here = ((lax.div(row, rows) * plane + p) * 2 + c) * rows + lax.rem(row, rows)
        ids.append(jnp.sum(jnp.where(lane == here, aid_ref[...].astype(F32), 0.0), axis=1, keepdims=True))
    ids = jnp.broadcast_to(jnp.concatenate(ids, axis=0), (group, LANES)).astype(jnp.int32)
    id_hi = lax.div(ids, per)
    id_lo = ids - id_hi * per
    tag_ref[...] = id_hi.astype(F32).astype(BF16)
    tag_t[...] = id_hi.astype(F32).T.astype(BF16)
    lane_g = lax.broadcasted_iota(jnp.int32, (group, LANES), 1)
    keep_ref[...] = jnp.where(lax.div(lane_g, RANK) == id_lo, 1.0, 0.0)

    for k in range(1, line):
        relay(k)
    for k in range(line // 2):
        receive(k)
    all_col.wait_recv()
    local[0].wait()
    adn_copy.wait_recv()
    cols = col[...].reshape(group, LANES)
    blocks = bank // LANES

    def masked(v, t, k):
        return jnp.where(t == jnp.asarray(k, BF16), v, jnp.zeros_like(v))

    tag = tag_ref[...]

    terms = jnp.zeros((group, LANES), F32)
    for k in range(0, blocks, 2):
        wide = jnp.concatenate([masked(cols, tag, k), masked(cols, tag, k + 1)], axis=1)
        tall = jnp.concatenate([adn[:, k * LANES : (k + 1) * LANES], adn[:, (k + 1) * LANES : (k + 2) * LANES]], axis=0)
        terms = terms + jnp.dot(wide, tall, preferred_element_type=F32)
    terms = (terms * keep_ref[...]).astype(BF16)
    fi = lax.broadcasted_iota(jnp.int32, (LANES, LANES), 0)
    fj = lax.broadcasted_iota(jnp.int32, (LANES, LANES), 1)
    fold = jnp.where(lax.rem(fi, RANK) == lax.rem(fj, RANK), 1.0, 0.0).astype(BF16)
    turn = lax.div(lane_g, RANK) == lax.rem(lax.broadcasted_iota(jnp.int32, (group, LANES), 0), per)
    folded = jnp.where(turn, jnp.dot(terms, fold, preferred_element_type=F32), 0.0)
    lr_send[...] = jnp.sum(folded.reshape(group // per, per, LANES), axis=1)
    lr1_recv[pl.ds(g, 1)] = lr_send[...].reshape(1, group // per, LANES)
    plane_peers(lambda d: lr1_copy(d, g).start())

    for k in range(line // 2, line):
        receive(k)
    for k in range(line - 1):
        multiply(k)
    multiply(line - 1)
    local[4].wait()

    def down_part(i):
        y = jnp.dot(hid[...], wd[:, chunk_of(turn_of(i, z))], preferred_element_type=F32)
        sib_send[i] = y[slots:].reshape(plane, line, cap, wide_n).astype(BF16)
        sib_copy(i).start()
        y_own[i] = y[:slots]

    def finish(i):
        sib_copy(i).wait_recv()
        ret_send[i] = (y_own[i].reshape(plane, line, cap, wide_n) + sib_recv[i].astype(F32)).astype(BF16)
        ret_recv[i, pl.ds(g, 1)] = ret_send[i, pl.ds(g, 1)]
        plane_peers(lambda d: ret_copy(i, d, g).start())

    for i in range(line):
        down_part(i)
    all_lr1.wait_recv()
    lr2_send[...] = jnp.sum(lr1_recv[...], axis=0)
    lr2_recv[pl.ds(z, 1)] = lr2_send[...].reshape(1, group // per, LANES)
    line_far(lambda d: lr2_copy(d, z).start())
    for i in range(line):
        finish(i)

    all_lr2.wait_recv()
    local[3].wait()
    aup_copy.wait_recv()
    low = jnp.sum(lr2_recv[...], axis=0).astype(BF16).astype(F32)
    ranks = jnp.broadcast_to(low.reshape(group // per, 1, LANES), (group // per, per, LANES)).reshape(group, LANES)
    ranks = jnp.where(turn, ranks, 0.0).astype(BF16)
    ranks = jnp.dot(ranks, fold, preferred_element_type=F32) * keep_ref[...]
    ranks = ranks.T.astype(BF16)
    tag = tag_t[...]
    corr = jnp.zeros((LANES, group), F32)
    for k in range(0, blocks, 2):
        tall = jnp.concatenate([masked(ranks, tag, k), masked(ranks, tag, k + 1)], axis=0)
        corr = corr + jnp.dot(aup[:, k * LANES : (k + 2) * LANES], tall, preferred_element_type=F32)
    cor_send[...] = corr.T.astype(BF16).reshape(plane, line, rows, LANES)
    cor_recv[pl.ds(g, 1)] = cor_send[pl.ds(g, 1)]
    plane_peers(lambda d: cor_copy(d, g).start())

    share = LANES // (2 * feats)

    def mix(i):
        some_ret(i).wait_recv()
        j = turn_of(i, z)
        if i == line - 1:
            all_cor.wait_recv()
        for s in range(line):
            back = ret_recv[i, :, s].astype(F32).reshape(block, wide_n).astype(BF16)
            both = line_comb[s]
            routed = jnp.dot(both[:, :block], back, preferred_element_type=F32)
            routed = routed + jnp.dot(both[:, half_l : half_l + block], back, preferred_element_type=F32)
            if i == line - 1:
                delta = []
                for b in range(wide_n // LANES):
                    one = cor_recv[b * share, s].astype(F32)
                    for t in range(1, share):
                        one = one + cor_recv[b * share + t, s].astype(F32)
                    delta.append(one)
                routed = routed + jnp.concatenate(delta, axis=1)
            part_send[i, s] = routed.astype(BF16)
        own_part[pl.ds(j, 1)] = part_send[i, pl.ds(z, 1)].astype(F32)
        line_far(lambda d: part_copy(i, d, z, j).start())

    for i in range(line):
        mix(i)

    for cp in (all_x, all_comb, all_col, all_disp, all_lr1, all_lr2, all_cor, all_ret):
        cp.wait_send()
    adn_copy.wait_send()
    aup_copy.wait_send()
    for i in range(line):
        sib_copy(i).wait_send()
        fwd_copy(i).wait_send()
    all_part.wait_recv()
    for j in range(line):
        def add(s, acc):
            return acc + part_recv[far(s), j].astype(F32)

        out_ref[:, j * wide_n : (j + 1) * wide_n] = lax.fori_loop(0, line - 1, add, own_part[j]).astype(BF16)

    out_copy = pltpu.make_async_copy(out_ref, out_hbm, out_sem.at[0])
    out_copy.start()
    all_part.wait_send()
    out_copy.wait()


def per_device(tokens, idx, gates, aid, wg, wu, wd, adn, aup):
    devices = lax.axis_size("exp")
    chips = devices // 2
    plane = 1
    while plane * plane < chips:
        plane *= 2
    line = chips // plane
    rows, width = tokens.shape
    top = idx.shape[1]
    half = wd.shape[1]
    feats, bank = adn.shape
    need = 2 * (rows * top // devices + 1)
    cap = -(-need // 8) * 8
    slots = chips * cap
    group = chips * rows
    short = chips * rows * RANK // LANES
    wide_n = width // line
    blocks = lambda *s: pltpu.VMEM(s, BF16)
    full = lambda *s: pltpu.VMEM(s, F32)
    sems = lambda n: pltpu.SemaphoreType.DMA((n,))
    hbm = pl.BlockSpec(memory_space=pl.ANY)
    return pl.pallas_call(
        functools.partial(kernel, line, plane, cap, top),
        out_shape=jax.ShapeDtypeStruct((rows, width), BF16),
        in_specs=[hbm] * 9,
        out_specs=hbm,
        scratch_shapes=[
            blocks(rows, width), pltpu.VMEM((top, rows), jnp.int32), full(top, rows), pltpu.VMEM((1, aid.shape[0]), jnp.int32),
            blocks(half, width), blocks(half, width), blocks(half, width),
            blocks(LANES, bank), blocks(LANES, bank),
            blocks(line, rows, width), blocks(line, rows, LANES), blocks(line, rows, LANES),
            blocks(line, plane * cap, rows),
            blocks(plane, line, rows, LANES),
            blocks(plane, line, cap, width), blocks(plane, line, cap, width), blocks(plane, line, cap, width),
            blocks(2 * slots, width), full(half, 2 * slots), full(half, 2 * slots), blocks(2 * slots, half),
            full(line, slots, wide_n),
            blocks(line, plane, line, cap, wide_n), blocks(line, plane, line, cap, wide_n),
            blocks(group, LANES), blocks(LANES, group), full(group, LANES),
            full(short, LANES), full(plane, short, LANES), full(short, LANES), full(line, short, LANES),
            blocks(plane, line, rows, LANES), blocks(plane, line, rows, LANES),
            blocks(line, plane, line, cap, wide_n), blocks(line, plane, line, cap, wide_n),
            blocks(line, line, rows, wide_n), blocks(line, line, rows, wide_n), full(line, rows, wide_n),
            sems(4), sems(1), sems(3), sems(2), sems(2), sems(2),
            sems(1), sems(line * line), sems(1), sems(line), sems(1), sems(1), sems(1), sems(line), sems(line), sems(line),
            sems(1), sems(1), sems(1), sems(1), sems(1), sems(1), sems(1), sems(line), sems(1), sems(1),
            sems(line), sems(line),
        ],
        compiler_params=pltpu.CompilerParams(
            collective_id=0, has_side_effects=True, vmem_limit_bytes=60 * 1024 * 1024
        ),
    )(tokens, idx.T, gates.T, aid.reshape(1, -1), wg.swapaxes(1, 2), wu.swapaxes(1, 2), wd, adn, aup)


def solution(mesh):
    placed = (
        P(("grp", "exp"), None),
        P(("grp", "exp"), None),
        P(("grp", "exp"), None),
        P("grp"),
        P("exp", None, None),
        P("exp", None, None),
        P("exp", None, None),
        P("exp", None),
        P("exp", None),
    )
    return jax.shard_map(
        per_device, mesh=mesh, in_specs=placed, out_specs=P(("grp", "exp"), None), check_vma=False
    )
```

```python
import functools

import jax
import jax.numpy as jnp
from jax import lax
from jax.experimental import pallas as pl
from jax.experimental.pallas import tpu as pltpu
from jax.sharding import PartitionSpec as P

RANK = 16
LANES = 128
BF16 = jnp.bfloat16
F32 = jnp.float32
MESH = pl.DeviceIdType.MESH


def dot_nt(a, b):
    return lax.dot_general(a, b, (((1,), (1,)), ((), ())), preferred_element_type=F32)


def kernel(
    line, plane, cap, top, x_hbm, idx_hbm, gate_hbm, aid_hbm, wg_hbm, wu_hbm, wd_hbm, adn_hbm, aup_hbm, out_ref,
    idx_ref, gate_ref, aid_ref, wg, wu, wd, adn, aup, line_x, comb_send, line_comb, pick_ref, col, disp, recv_a,
    recv_b, xs, gt_ref, up_ref, hid, sib_send, sib_recv, tag_ref, tag_t, keep_ref, lr_send, lr1_recv, lr2_send,
    lr2_recv, cor_send, cor_recv, ret_send, ret_recv, part_send, part_recv, own_part, in_sem, w_sem, adl_sem, ad_s,
    ad_r, x_s, x_r, cb_s, cb_r, col_s, col_r, disp_s, disp_r, fwd_s, fwd_r, l1_s, l1_r, l2_s, l2_r, cor_s, cor_r,
    ret_s, ret_r, part_s, part_r, sib_s, sib_r,
):
    me = lax.axis_index("exp")
    q = lax.div(me, 2)
    c = lax.rem(me, 2)
    z = lax.div(q, plane)
    g = lax.rem(q, plane)
    sib = me + 1 - 2 * c
    rows, width = x_hbm.shape
    feats = adn_hbm.shape[0]
    bank = adn_hbm.shape[1]
    chips = line * plane
    group = chips * rows
    slots = chips * cap
    block = plane * cap
    wide_n = width // line
    off = pl.multiple_of(lax.rem(me * feats, LANES), feats)
    half_l = LANES // 2

    def remote(src, dst, ss, rs, dev):
        return pltpu.make_async_remote_copy(
            src_ref=src, dst_ref=dst, send_sem=ss, recv_sem=rs, device_id={"exp": dev}, device_id_type=MESH
        )

    def dev_z(to):
        return 2 * (to * plane + g) + c

    def dev_g(to):
        return 2 * (z * plane + to) + c

    def dev_cross(to):
        return 2 * (z * plane + to) + 1 - c

    side = lax.div(2 * z, line)
    mirror = side * z + (1 - side) * (line - 1 - z)

    def far(s):
        d = s + lax.div(s - mirror + line, line)
        return side * d + (1 - side) * (line - 1 - d)

    def loop(n, fn):
        def step(r, carry):
            fn(r)
            return carry

        lax.fori_loop(0, n, step, 0)

    def line_far(fn):
        loop(line - 1, lambda s: fn(far(s)))

    def line_near(fn):
        loop(line - 1, lambda s: fn(far(line - 2 - s)))

    def plane_peers(fn):
        loop(plane - 1, lambda r: fn(lax.rem(g + 1 + r, plane)))

    barrier = pltpu.get_barrier_semaphore()
    if 2 * feats < LANES:
        adn[...] = jnp.zeros_like(adn)
        aup[...] = jnp.zeros_like(aup)

    def greet(dev):
        pl.semaphore_signal(barrier, inc=1, device_id={"exp": dev}, device_id_type=MESH)

    line_far(lambda d: greet(dev_z(d)))
    plane_peers(lambda d: greet(dev_g(d)))
    plane_peers(lambda d: greet(dev_cross(d)))
    greet(sib)

    own_rows = pl.ds(off, feats)
    inputs = [
        pltpu.make_async_copy(idx_hbm, idx_ref, in_sem.at[0]),
        pltpu.make_async_copy(gate_hbm, gate_ref, in_sem.at[1]),
        pltpu.make_async_copy(x_hbm, line_x.at[z], in_sem.at[2]),
        pltpu.make_async_copy(aid_hbm, aid_ref, in_sem.at[3]),
    ]
    for cp in inputs:
        cp.start()
    local = [
        pltpu.make_async_copy(adn_hbm, adn.at[own_rows], adl_sem.at[0]),
        pltpu.make_async_copy(wg_hbm.at[0], wg, w_sem.at[0]),
        pltpu.make_async_copy(wu_hbm.at[0], wu, w_sem.at[1]),
        pltpu.make_async_copy(aup_hbm, aup.at[own_rows], adl_sem.at[1]),
        pltpu.make_async_copy(wd_hbm.at[0], wd, w_sem.at[2]),
    ]
    for cp in inputs:
        cp.wait()
    for cp in local:
        cp.start()
    pl.semaphore_wait(barrier, line + 2 * plane - 2)

    def step_of(k, at):
        return at if k == 0 else k - 1 + lax.div(k - 1 + line - at, line)

    def lanes_of(chip):
        return pl.ds(pl.multiple_of(lax.div(chip * 2 * feats, LANES) * LANES, LANES), LANES)

    def chunk_of(i):
        return pl.ds(pl.multiple_of(i * wide_n, wide_n), wide_n)

    def x_copy(to, slot, i, kind):
        at = chunk_of(i)
        return remote(line_x.at[z, :, at], line_x.at[slot, :, at], x_s.at[0], x_r.at[kind * line + slot], dev_z(to))

    def comb_copy(to, slot):
        return remote(comb_send.at[to], line_comb.at[slot], cb_s.at[0], cb_r.at[slot], dev_z(to))

    def col_copy(to, s):
        return remote(
            line_x.at[s, :, lanes_of(z * plane + to)], col.at[c, g, s],
            col_s.at[0], col_r.at[c], 2 * (z * plane + to) + 1,
        )

    def disp_copy(to, slot, s, k):
        at = chunk_of(step_of(k, z))
        return remote(disp.at[to, s, :, at], recv_a.at[slot, s, :, at], disp_s.at[0], disp_r.at[k], dev_g(to))

    def fwd_copy(k):
        at = chunk_of(step_of(k, z))
        return remote(recv_a.at[:, :, :, at], recv_b.at[:, :, :, at], fwd_s.at[k], fwd_r.at[k], sib)

    def lr1_copy(par, to):
        return remote(
            lr_send.at[par], lr1_recv.at[g], l1_s.at[par], l1_r.at[0], 2 * (z * plane + to) + par
        )

    def lr2_copy(to, slot):
        return remote(lr2_send, lr2_recv.at[slot], l2_s.at[0], l2_r.at[0], dev_z(to))

    def cor_copy(to, slot):
        return remote(cor_send.at[to], cor_recv.at[slot], cor_s.at[0], cor_r.at[0], dev_g(to))

    def ret_copy(i, to, slot):
        return remote(ret_send.at[i, to], ret_recv.at[i, slot], ret_s.at[0], ret_r.at[i], dev_g(to))

    def turn_of(i, at):
        return lax.rem(at + 1 + i, line)

    def part_copy(i, to, slot, j):
        return remote(part_send.at[i, to], part_recv.at[slot, j], part_s.at[0], part_r.at[0], dev_z(to))

    def sib_copy(i):
        return remote(sib_send.at[i], sib_recv.at[i], sib_s.at[i], sib_r.at[i], sib)

    rest_z = pl.ds(0, line - 1)
    rest_g = pl.ds(0, plane - 1)
    all_x = remote(line_x.at[rest_z], line_x.at[rest_z], x_s.at[0], x_r.at[0], sib)
    all_comb = remote(comb_send.at[rest_z], line_comb.at[rest_z], cb_s.at[0], cb_r.at[0], sib)
    some_col = remote(col.at[1, rest_g], col.at[1, rest_g], col_s.at[0], col_r.at[1], sib)
    all_col = remote(col.at[0], col.at[0], col_s.at[0], col_r.at[0], sib)
    all_disp = remote(disp.at[rest_g], recv_a.at[rest_g], disp_s.at[0], disp_r.at[0], sib)
    some_lr1 = remote(lr1_recv.at[rest_g], lr1_recv.at[rest_g], l1_s.at[1], l1_r.at[0], sib)
    all_lr1 = remote(lr1_recv, lr1_recv, l1_s.at[0], l1_r.at[0], sib)
    all_lr2 = remote(lr2_recv.at[rest_z], lr2_recv.at[rest_z], l2_s.at[0], l2_r.at[0], sib)
    all_cor = remote(cor_send.at[rest_g], cor_recv.at[rest_g], cor_s.at[0], cor_r.at[0], sib)
    all_ret = remote(ret_send.at[:, rest_g], ret_recv.at[:, rest_g], ret_s.at[0], ret_r.at[0], sib)
    all_part = remote(part_send.at[:, rest_z], part_recv.at[rest_z], part_s.at[0], part_r.at[0], sib)

    def some_x(s, k):
        at = chunk_of(0)
        return remote(line_x.at[s, :, at], line_x.at[s, :, at], x_s.at[0], x_r.at[k * line + s], sib)

    def some_disp(k):
        at = chunk_of(0)
        return remote(disp.at[rest_g, :, :, at], recv_a.at[rest_g, :, :, at], disp_s.at[0], disp_r.at[k], sib)

    def some_ret(i):
        return remote(ret_send.at[i, rest_g], ret_recv.at[i, rest_g], ret_s.at[0], ret_r.at[i], sib)

    line_far(lambda d: x_copy(d, z, step_of(0, d), 0).start())
    plane_peers(lambda d: col_copy(d, z).start())
    slot = lax.broadcasted_iota(jnp.int32, (slots, rows), 0)
    slot_e = lax.div(slot, cap)
    chosen = jnp.zeros((slots, rows), F32)
    weight = jnp.zeros((slots, rows), F32)
    for k in range(top):
        hit = idx_ref[k : k + 1, :] == slot_e
        chosen = chosen + jnp.where(hit, 1.0, 0.0)
        weight = weight + jnp.where(hit, gate_ref[k : k + 1, :], 0.0)
    earlier = jnp.where(
        lax.broadcasted_iota(jnp.int32, (rows, rows), 0) < lax.broadcasted_iota(jnp.int32, (rows, rows), 1), 1.0, 0.0
    )
    rank_of = jnp.dot(chosen.astype(BF16), earlier.astype(BF16), preferred_element_type=F32)
    slot_p = lax.rem(slot, cap).astype(F32)
    combine = jnp.where((chosen > 0.5) & (rank_of == slot_p), weight, 0.0)
    for d in range(line):
        part = combine[d * block : (d + 1) * block].T
        hi = part.astype(BF16)
        lo = (part - hi.astype(F32)).astype(BF16)
        comb_send[d, :, :block] = hi
        comb_send[d, :, half_l : half_l + block] = lo
    line_comb[pl.ds(z, 1)] = comb_send[pl.ds(z, 1)]

    line_far(lambda d: comb_copy(d, z).start())
    for k in range(1, line):
        line_far(lambda d: x_copy(d, z, step_of(k, d), k).start())
    adn_copy = remote(adn_hbm, adn.at[own_rows], ad_s.at[0], ad_r.at[0], sib)
    aup_copy = remote(aup_hbm, aup.at[own_rows], ad_s.at[1], ad_r.at[1], sib)
    adn_copy.start()
    aup_copy.start()

    def own_col(s):
        @pl.when(c == 1)
        def _():
            col[1, pl.ds(g, 1), pl.ds(s, 1)] = line_x[pl.ds(s, 1), :, lanes_of(q)].reshape(1, 1, rows, LANES)

        @pl.when(c == 0)
        def _():
            col_copy(g, s).start()

    def take_pick(s):
        pick = jnp.where(line_comb[s].astype(F32) > 0.0, 1.0, 0.0).T[:block]
        pick_ref[pl.ds(s, 1)] = pick.astype(BF16).reshape(1, block, rows)

    def pack(s, k):
        at = chunk_of(step_of(k, z))
        packed = jnp.dot(pick_ref[s], line_x[s, :, at], preferred_element_type=F32)
        disp[:, pl.ds(s, 1), :, at] = packed.reshape(plane, 1, cap, wide_n).astype(BF16)
        recv_a[pl.ds(g, 1), pl.ds(s, 1), :, at] = disp[pl.ds(g, 1), pl.ds(s, 1), :, at]
        plane_peers(lambda d: disp_copy(d, g, s, k).start())

    take_pick(z)
    for k in range(line):
        pack(z, k)
    own_col(z)

    near_z = [far(line - 2 - k) for k in range(line - 1)]
    half = wd.shape[0]
    cut = -(-half // (2 * LANES)) * LANES

    def relay(k):
        for s in near_z:
            some_x(s, k).wait_recv()
            if k == 0:
                plane_peers(lambda d: col_copy(d, s).start())
                own_col(s)
                comb_copy(z, s).wait_recv()
                take_pick(s)
            pack(s, k)

    def receive(k):
        at = chunk_of(step_of(k, z))
        some_disp(k).wait_recv()
        fwd_copy(k).start()
        xs[:slots, at] = recv_a[:, :, :, at].astype(F32).reshape(slots, wide_n).astype(BF16)

    def multiply(k):
        at = chunk_of(step_of(k, z))
        fwd_copy(k).wait_recv()
        xs[slots:, at] = recv_b[:, :, :, at].astype(F32).reshape(slots, wide_n).astype(BF16)
        if k == 0:
            local[1].wait()
            local[2].wait()
        for a, b in ((0, cut), (cut, half)):
            gt = dot_nt(wg[a:b, at], xs[:, at])
            up = dot_nt(wu[a:b, at], xs[:, at])
            if k > 0:
                gt = gt + gt_ref[a:b]
                up = up + up_ref[a:b]
            if k < line - 1:
                gt_ref[a:b] = gt
                up_ref[a:b] = up
            else:
                hid[:, a:b] = (gt / (1.0 + jnp.exp(-gt)) * up).T.astype(BF16)

    per = LANES // RANK
    near = line * rows
    lane_g = lax.broadcasted_iota(jnp.int32, (group, LANES), 1)
    own = jnp.zeros((group, LANES), jnp.int32)
    for par in range(2):
        ids = []
        for p in range(plane):
            lane = lax.broadcasted_iota(jnp.int32, (near, aid_ref.shape[1]), 1)
            row = lax.broadcasted_iota(jnp.int32, (near, aid_ref.shape[1]), 0)
            here = ((lax.div(row, rows) * plane + p) * 2 + par) * rows + lax.rem(row, rows)
            ids.append(jnp.sum(jnp.where(lane == here, aid_ref[...].astype(F32), 0.0), axis=1, keepdims=True))
        ids = jnp.broadcast_to(jnp.concatenate(ids, axis=0), (group, LANES)).astype(jnp.int32)
        id_hi = lax.div(ids, per)
        tag_ref[par] = id_hi.astype(F32).astype(BF16)
        keep_ref[par] = jnp.where(lax.div(lane_g, RANK) == ids - id_hi * per, 1.0, 0.0)
        own = jnp.where(c == par, id_hi, own)
    tag_t[...] = own.astype(F32).T.astype(BF16)
    relay(0)
    for k in range(1, line):
        relay(k)
    blocks = bank // LANES

    def masked(v, t, k):
        return jnp.where(t == jnp.asarray(k, BF16), v, jnp.zeros_like(v))

    fi = lax.broadcasted_iota(jnp.int32, (LANES, LANES), 0)
    fj = lax.broadcasted_iota(jnp.int32, (LANES, LANES), 1)
    fold = jnp.where(lax.rem(fi, RANK) == lax.rem(fj, RANK), 1.0, 0.0).astype(BF16)
    turn = lax.div(lane_g, RANK) == lax.rem(lax.broadcasted_iota(jnp.int32, (group, LANES), 0), per)

    def down(par):
        cols = col[par].reshape(group, LANES)
        tag = tag_ref[par]
        terms = jnp.zeros((group, LANES), F32)
        for k in range(0, blocks, 2):
            wide = jnp.concatenate([masked(cols, tag, k), masked(cols, tag, k + 1)], axis=1)
            tall = jnp.concatenate(
                [adn[:, k * LANES : (k + 1) * LANES], adn[:, (k + 1) * LANES : (k + 2) * LANES]], axis=0
            )
            terms = terms + jnp.dot(wide, tall, preferred_element_type=F32)
        terms = (terms * keep_ref[par]).astype(BF16)
        folded = jnp.where(turn, jnp.dot(terms, fold, preferred_element_type=F32), 0.0)
        lr_send[par] = jnp.sum(folded.reshape(group // per, per, LANES), axis=1).astype(BF16)
        plane_peers(lambda d: lr1_copy(par, d).start())

    local[0].wait()
    adn_copy.wait_recv()

    @pl.when(c == 1)
    def _():
        some_col.wait_recv()
        down(1)
        lr1_recv[pl.ds(g, 1)] = lr_send[1].reshape(1, group // per, LANES)

    for k in range(line // 2):
        receive(k)
    for k in range(line // 2, line):
        receive(k)
    @pl.when(c == 1)
    def _():
        all_col.wait_recv()
        down(0)
        lr1_copy(0, g).start()

    for k in range(line - 1):
        multiply(k)
    multiply(line - 1)
    local[4].wait()

    def down_sib(i):
        at = chunk_of(turn_of(i, z))
        y = jnp.dot(hid[slots:], wd[:, at], preferred_element_type=F32)
        sib_send[i] = y.reshape(plane, line, cap, wide_n).astype(BF16)
        sib_copy(i).start()

    def finish(i):
        at = chunk_of(turn_of(i, z))
        y = jnp.dot(hid[:slots], wd[:, at], preferred_element_type=F32).reshape(plane, line, cap, wide_n)
        sib_copy(i).wait_recv()
        ret_send[i] = (y + sib_recv[i].astype(F32)).astype(BF16)
        ret_recv[i, pl.ds(g, 1)] = ret_send[i, pl.ds(g, 1)]
        plane_peers(lambda d: ret_copy(i, d, g).start())

    for i in range(line):
        down_sib(i)
    @pl.when(c == 1)
    def _():
        some_lr1.wait_recv()

    @pl.when(c == 0)
    def _():
        all_lr1.wait_recv()

    lr2_send[...] = jnp.sum(lr1_recv[...].astype(F32), axis=0).astype(BF16)
    lr2_recv[pl.ds(z, 1)] = lr2_send[...].reshape(1, group // per, LANES)
    line_far(lambda d: lr2_copy(d, z).start())
    for i in range(line):
        finish(i)

    all_lr2.wait_recv()
    local[3].wait()
    aup_copy.wait_recv()
    low = jnp.sum(lr2_recv[...].astype(F32), axis=0).astype(BF16).astype(F32)
    ranks = jnp.broadcast_to(low.reshape(group // per, 1, LANES), (group // per, per, LANES)).reshape(group, LANES)
    ranks = jnp.where(turn, ranks, 0.0).astype(BF16)
    ranks = jnp.dot(ranks, fold, preferred_element_type=F32) * keep_ref[c]
    ranks = ranks.T.astype(BF16)
    tag = tag_t[...]
    corr = jnp.zeros((LANES, group), F32)
    for k in range(0, blocks, 2):
        tall = jnp.concatenate([masked(ranks, tag, k), masked(ranks, tag, k + 1)], axis=0)
        corr = corr + jnp.dot(aup[:, k * LANES : (k + 2) * LANES], tall, preferred_element_type=F32)
    cor_send[...] = corr.T.astype(BF16).reshape(plane, line, rows, LANES)
    cor_recv[pl.ds(g, 1)] = cor_send[pl.ds(g, 1)]
    plane_peers(lambda d: cor_copy(d, g).start())

    share = LANES // (2 * feats)

    def mix(i):
        some_ret(i).wait_recv()
        j = turn_of(i, z)
        if i == line - 1:
            all_cor.wait_recv()
        for s in range(line):
            back = ret_recv[i, :, s].astype(F32).reshape(block, wide_n).astype(BF16)
            both = line_comb[s]
            routed = jnp.dot(both[:, :block], back, preferred_element_type=F32)
            routed = routed + jnp.dot(both[:, half_l : half_l + block], back, preferred_element_type=F32)
            if i == line - 1:
                delta = []
                for b in range(wide_n // LANES):
                    one = cor_recv[b * share, s].astype(F32)
                    for t in range(1, share):
                        one = one + cor_recv[b * share + t, s].astype(F32)
                    delta.append(one)
                routed = routed + jnp.concatenate(delta, axis=1)
            part_send[i, s] = routed.astype(BF16)
        own_part[pl.ds(j, 1)] = part_send[i, pl.ds(z, 1)].astype(F32)
        line_far(lambda d: part_copy(i, d, z, j).start())

    for i in range(line):
        mix(i)

    for cp in (all_x, all_comb, all_disp, all_lr2, all_cor, all_ret):
        cp.wait_send()

    @pl.when(c == 1)
    def _():
        some_col.wait_send()
        some_lr1.wait_send()
        all_lr1.wait_send()

    @pl.when(c == 0)
    def _():
        all_col.wait_send()

    adn_copy.wait_send()
    aup_copy.wait_send()
    for i in range(line):
        sib_copy(i).wait_send()
        fwd_copy(i).wait_send()
    all_part.wait_recv()
    for j in range(line):
        def add(s, acc):
            return acc + part_recv[far(s), j].astype(F32)

        out_ref[:, j * wide_n : (j + 1) * wide_n] = lax.fori_loop(0, line - 1, add, own_part[j]).astype(BF16)

    all_part.wait_send()


def per_device(tokens, idx, gates, aid, wg, wu, wd, adn, aup):
    devices = lax.axis_size("exp")
    chips = devices // 2
    plane = 1
    while plane * plane < chips:
        plane *= 2
    line = chips // plane
    rows, width = tokens.shape
    top = idx.shape[1]
    half = wd.shape[1]
    feats, bank = adn.shape
    need = 2 * (rows * top // devices + 1)
    cap = -(-need // 8) * 8
    slots = chips * cap
    group = chips * rows
    short = chips * rows * RANK // LANES
    wide_n = width // line
    blocks = lambda *s: pltpu.VMEM(s, BF16)
    full = lambda *s: pltpu.VMEM(s, F32)
    sems = lambda n: pltpu.SemaphoreType.DMA((n,))
    hbm = pl.BlockSpec(memory_space=pl.ANY)
    return pl.pallas_call(
        functools.partial(kernel, line, plane, cap, top),
        out_shape=pltpu.VMEM((rows, width), BF16),
        in_specs=[hbm] * 9,
        out_specs=pl.BlockSpec(memory_space=pltpu.VMEM),
        scratch_shapes=[
            pltpu.VMEM((top, rows), jnp.int32), full(top, rows), pltpu.VMEM((1, aid.shape[0]), jnp.int32),
            blocks(half, width), blocks(half, width), blocks(half, width),
            blocks(LANES, bank), blocks(LANES, bank),
            blocks(line, rows, width), blocks(line, rows, LANES), blocks(line, rows, LANES),
            blocks(line, plane * cap, rows),
            blocks(2, plane, line, rows, LANES),
            blocks(plane, line, cap, width), blocks(plane, line, cap, width), blocks(plane, line, cap, width),
            blocks(2 * slots, width), full(half, 2 * slots), full(half, 2 * slots), blocks(2 * slots, half),
            blocks(line, plane, line, cap, wide_n), blocks(line, plane, line, cap, wide_n),
            blocks(2, group, LANES), blocks(LANES, group), full(2, group, LANES),
            blocks(2, short, LANES), blocks(plane, short, LANES), blocks(short, LANES), blocks(line, short, LANES),
            blocks(plane, line, rows, LANES), blocks(plane, line, rows, LANES),
            blocks(line, plane, line, cap, wide_n), blocks(line, plane, line, cap, wide_n),
            blocks(line, line, rows, wide_n), blocks(line, line, rows, wide_n), full(line, rows, wide_n),
            sems(4), sems(3), sems(2), sems(2), sems(2),
            sems(1), sems(line * line), sems(1), sems(line), sems(1), sems(2), sems(1), sems(line), sems(line), sems(line),
            sems(2), sems(1), sems(1), sems(1), sems(1), sems(1), sems(1), sems(line), sems(1), sems(1),
            sems(line), sems(line),
        ],
        compiler_params=pltpu.CompilerParams(
            collective_id=0, has_side_effects=True, vmem_limit_bytes=62 * 1024 * 1024
        ),
    )(tokens, idx.T, gates.T, aid.reshape(1, -1), wg.swapaxes(1, 2), wu.swapaxes(1, 2), wd, adn, aup)


def solution(mesh):
    placed = (
        P(("grp", "exp"), None),
        P(("grp", "exp"), None),
        P(("grp", "exp"), None),
        P("grp"),
        P("exp", None, None),
        P("exp", None, None),
        P("exp", None, None),
        P("exp", None),
        P("exp", None),
    )
    return jax.shard_map(
        per_device, mesh=mesh, in_specs=placed, out_specs=P(("grp", "exp"), None), check_vma=False
    )
```

```python
import functools

import jax
import jax.numpy as jnp
from jax import lax
from jax.experimental import pallas as pl
from jax.experimental.pallas import tpu as pltpu
from jax.sharding import PartitionSpec as P

RANK = 16
LANES = 128
BF16 = jnp.bfloat16
F32 = jnp.float32
MESH = pl.DeviceIdType.MESH


def dot_nt(a, b):
    return lax.dot_general(a, b, (((1,), (1,)), ((), ())), preferred_element_type=F32)


def kernel(
    line, plane, cap, top, x_hbm, idx_hbm, gate_hbm, aid_hbm, wg_hbm, wu_hbm, wd_hbm, adn_hbm, aup_hbm, out_ref,
    idx_ref, gate_ref, aid_ref, wg, wu, wd, adn, aup, line_x, comb_send, line_comb, pick_ref, col, disp, recv_a,
    recv_b, xs, gt_ref, up_ref, hid, sib_send, sib_recv, tag_ref, tag_t, keep_ref, lr_send, lr1_recv, lr2_send,
    lr2_recv, cor_send, cor_recv, ret_send, ret_recv, part_send, part_recv, own_part, in_sem, w_sem, adl_sem, ad_s,
    ad_r, x_s, x_r, cb_s, cb_r, col_s, col_r, disp_s, disp_r, fwd_s, fwd_r, l1_s, l1_r, l2_s, l2_r, cor_s, cor_r,
    ret_s, ret_r, part_s, part_r, sib_s, sib_r,
):
    me = lax.axis_index("exp")
    q = lax.div(me, 2)
    c = lax.rem(me, 2)
    z = lax.div(q, plane)
    g = lax.rem(q, plane)
    sib = me + 1 - 2 * c
    rows, width = x_hbm.shape
    feats = adn_hbm.shape[0]
    bank = adn_hbm.shape[1]
    chips = line * plane
    group = chips * rows
    slots = chips * cap
    block = plane * cap
    wide_n = width // line
    off = pl.multiple_of(lax.rem(me * feats, LANES), feats)
    half_l = LANES // 2

    def remote(src, dst, ss, rs, dev):
        return pltpu.make_async_remote_copy(
            src_ref=src, dst_ref=dst, send_sem=ss, recv_sem=rs, device_id={"exp": dev}, device_id_type=MESH
        )

    def dev_z(to):
        return 2 * (to * plane + g) + c

    def dev_g(to):
        return 2 * (z * plane + to) + c

    def dev_cross(to):
        return 2 * (z * plane + to) + 1 - c

    side = lax.div(2 * z, line)
    mirror = side * z + (1 - side) * (line - 1 - z)

    def far(s):
        d = s + lax.div(s - mirror + line, line)
        return side * d + (1 - side) * (line - 1 - d)

    def loop(n, fn):
        def step(r, carry):
            fn(r)
            return carry

        lax.fori_loop(0, n, step, 0)

    def line_far(fn):
        loop(line - 1, lambda s: fn(far(s)))

    def line_near(fn):
        loop(line - 1, lambda s: fn(far(line - 2 - s)))

    def plane_peers(fn):
        loop(plane - 1, lambda r: fn(lax.rem(g + 1 + r, plane)))

    barrier = pltpu.get_barrier_semaphore()
    if 2 * feats < LANES:
        adn[...] = jnp.zeros_like(adn)
        aup[...] = jnp.zeros_like(aup)

    def greet(dev):
        pl.semaphore_signal(barrier, inc=1, device_id={"exp": dev}, device_id_type=MESH)

    line_far(lambda d: greet(dev_z(d)))
    plane_peers(lambda d: greet(dev_g(d)))
    plane_peers(lambda d: greet(dev_cross(d)))
    greet(sib)

    own_rows = pl.ds(off, feats)
    inputs = [
        pltpu.make_async_copy(idx_hbm, idx_ref, in_sem.at[0]),
        pltpu.make_async_copy(gate_hbm, gate_ref, in_sem.at[1]),
        pltpu.make_async_copy(x_hbm, line_x.at[z], in_sem.at[2]),
        pltpu.make_async_copy(aid_hbm, aid_ref, in_sem.at[3]),
    ]
    for cp in inputs:
        cp.start()
    local = [
        pltpu.make_async_copy(adn_hbm, adn.at[own_rows], adl_sem.at[0]),
        pltpu.make_async_copy(wg_hbm.at[0], wg, w_sem.at[0]),
        pltpu.make_async_copy(wu_hbm.at[0], wu, w_sem.at[1]),
        pltpu.make_async_copy(aup_hbm, aup.at[own_rows], adl_sem.at[1]),
        pltpu.make_async_copy(wd_hbm.at[0], wd, w_sem.at[2]),
    ]
    for cp in inputs:
        cp.wait()
    for cp in local:
        cp.start()
    pl.semaphore_wait(barrier, line + 2 * plane - 2)

    def step_of(k, at):
        return at if k == 0 else k - 1 + lax.div(k - 1 + line - at, line)

    def lanes_of(chip):
        return pl.ds(pl.multiple_of(lax.div(chip * 2 * feats, LANES) * LANES, LANES), LANES)

    def chunk_of(i):
        return pl.ds(pl.multiple_of(i * wide_n, wide_n), wide_n)

    def x_copy(to, slot, i, kind):
        at = chunk_of(i)
        return remote(line_x.at[z, :, at], line_x.at[slot, :, at], x_s.at[0], x_r.at[kind * line + slot], dev_z(to))

    def comb_copy(to, slot):
        return remote(comb_send.at[to], line_comb.at[slot], cb_s.at[0], cb_r.at[slot], dev_z(to))

    def col_copy(to, s):
        return remote(
            line_x.at[s, :, lanes_of(z * plane + to)], col.at[c, g, s],
            col_s.at[0], col_r.at[c], 2 * (z * plane + to) + 1,
        )

    def disp_copy(to, slot, s, k):
        at = chunk_of(step_of(k, z))
        return remote(disp.at[to, s, :, at], recv_a.at[slot, s, :, at], disp_s.at[0], disp_r.at[k], dev_g(to))

    def fwd_copy(k):
        at = chunk_of(step_of(k, z))
        return remote(recv_a.at[:, :, :, at], recv_b.at[:, :, :, at], fwd_s.at[k], fwd_r.at[k], sib)

    def lr1_copy(par, to):
        return remote(
            lr_send.at[par], lr1_recv.at[g], l1_s.at[par], l1_r.at[0], 2 * (z * plane + to) + par
        )

    def lr2_copy(to, slot):
        return remote(lr2_send, lr2_recv.at[slot], l2_s.at[0], l2_r.at[0], dev_z(to))

    def cor_copy(to, slot):
        return remote(cor_send.at[to], cor_recv.at[slot], cor_s.at[0], cor_r.at[0], dev_g(to))

    def ret_copy(i, to, slot):
        return remote(ret_send.at[i, to], ret_recv.at[i, slot], ret_s.at[0], ret_r.at[i], dev_g(to))

    def turn_of(i, at):
        return lax.rem(at + 1 + i, line)

    def part_copy(i, to, slot, j):
        return remote(part_send.at[i, to], part_recv.at[slot, j], part_s.at[0], part_r.at[0], dev_z(to))

    def sib_copy(i):
        return remote(sib_send.at[i], sib_recv.at[i], sib_s.at[i], sib_r.at[i], sib)

    rest_z = pl.ds(0, line - 1)
    rest_g = pl.ds(0, plane - 1)
    all_x = remote(line_x.at[rest_z], line_x.at[rest_z], x_s.at[0], x_r.at[0], sib)
    all_comb = remote(comb_send.at[rest_z], line_comb.at[rest_z], cb_s.at[0], cb_r.at[0], sib)
    some_col = remote(col.at[1, rest_g], col.at[1, rest_g], col_s.at[0], col_r.at[1], sib)
    all_col = remote(col.at[0], col.at[0], col_s.at[0], col_r.at[0], sib)
    all_disp = remote(disp.at[rest_g], recv_a.at[rest_g], disp_s.at[0], disp_r.at[0], sib)
    some_lr1 = remote(lr1_recv.at[rest_g], lr1_recv.at[rest_g], l1_s.at[1], l1_r.at[0], sib)
    all_lr1 = remote(lr1_recv, lr1_recv, l1_s.at[0], l1_r.at[0], sib)
    all_lr2 = remote(lr2_recv.at[rest_z], lr2_recv.at[rest_z], l2_s.at[0], l2_r.at[0], sib)
    all_cor = remote(cor_send.at[rest_g], cor_recv.at[rest_g], cor_s.at[0], cor_r.at[0], sib)
    all_ret = remote(ret_send.at[:, rest_g], ret_recv.at[:, rest_g], ret_s.at[0], ret_r.at[0], sib)
    all_part = remote(part_send.at[:, rest_z], part_recv.at[rest_z], part_s.at[0], part_r.at[0], sib)

    def some_x(s, k):
        at = chunk_of(0)
        return remote(line_x.at[s, :, at], line_x.at[s, :, at], x_s.at[0], x_r.at[k * line + s], sib)

    def some_disp(k):
        at = chunk_of(0)
        return remote(disp.at[rest_g, :, :, at], recv_a.at[rest_g, :, :, at], disp_s.at[0], disp_r.at[k], sib)

    def some_ret(i):
        return remote(ret_send.at[i, rest_g], ret_recv.at[i, rest_g], ret_s.at[0], ret_r.at[i], sib)

    line_far(lambda d: x_copy(d, z, step_of(0, d), 0).start())
    plane_peers(lambda d: col_copy(d, z).start())
    slot = lax.broadcasted_iota(jnp.int32, (slots, rows), 0)
    slot_e = lax.div(slot, cap)
    chosen = jnp.zeros((slots, rows), F32)
    weight = jnp.zeros((slots, rows), F32)
    for k in range(top):
        hit = idx_ref[k : k + 1, :] == slot_e
        chosen = chosen + jnp.where(hit, 1.0, 0.0)
        weight = weight + jnp.where(hit, gate_ref[k : k + 1, :], 0.0)
    earlier = jnp.where(
        lax.broadcasted_iota(jnp.int32, (rows, rows), 0) < lax.broadcasted_iota(jnp.int32, (rows, rows), 1), 1.0, 0.0
    )
    rank_of = jnp.dot(chosen.astype(BF16), earlier.astype(BF16), preferred_element_type=F32)
    slot_p = lax.rem(slot, cap).astype(F32)
    combine = jnp.where((chosen > 0.5) & (rank_of == slot_p), weight, 0.0)
    for d in range(line):
        part = combine[d * block : (d + 1) * block].T
        hi = part.astype(BF16)
        lo = (part - hi.astype(F32)).astype(BF16)
        comb_send[d, :, :block] = hi
        comb_send[d, :, half_l : half_l + block] = lo
    line_comb[pl.ds(z, 1)] = comb_send[pl.ds(z, 1)]

    line_far(lambda d: comb_copy(d, z).start())
    for k in range(1, line):
        line_far(lambda d: x_copy(d, z, step_of(k, d), k).start())
    adn_copy = remote(adn_hbm, adn.at[own_rows], ad_s.at[0], ad_r.at[0], sib)
    aup_copy = remote(aup_hbm, aup.at[own_rows], ad_s.at[1], ad_r.at[1], sib)
    adn_copy.start()
    aup_copy.start()

    def own_col(s):
        @pl.when(c == 1)
        def _():
            col[1, pl.ds(g, 1), pl.ds(s, 1)] = line_x[pl.ds(s, 1), :, lanes_of(q)].reshape(1, 1, rows, LANES)

        @pl.when(c == 0)
        def _():
            col_copy(g, s).start()

    def take_pick(s):
        pick = jnp.where(line_comb[s].astype(F32) != 0.0, 1.0, 0.0).T[:block]
        pick_ref[pl.ds(s, 1)] = pick.astype(BF16).reshape(1, block, rows)

    def pack(s, k):
        at = chunk_of(step_of(k, z))
        packed = jnp.dot(pick_ref[s], line_x[s, :, at], preferred_element_type=F32)
        disp[:, pl.ds(s, 1), :, at] = packed.reshape(plane, 1, cap, wide_n).astype(BF16)
        recv_a[pl.ds(g, 1), pl.ds(s, 1), :, at] = disp[pl.ds(g, 1), pl.ds(s, 1), :, at]
        plane_peers(lambda d: disp_copy(d, g, s, k).start())

    take_pick(z)
    for k in range(line):
        pack(z, k)
    own_col(z)

    near_z = [far(line - 2 - k) for k in range(line - 1)]
    half = wd.shape[0]
    cut = -(-half // (2 * LANES)) * LANES

    def relay(k):
        for s in near_z:
            some_x(s, k).wait_recv()
            if k == 0:
                plane_peers(lambda d: col_copy(d, s).start())
                own_col(s)
                comb_copy(z, s).wait_recv()
                take_pick(s)
            pack(s, k)

    def receive(k):
        at = chunk_of(step_of(k, z))
        some_disp(k).wait_recv()
        fwd_copy(k).start()
        xs[:slots, at] = recv_a[:, :, :, at].astype(F32).reshape(slots, wide_n).astype(BF16)

    def multiply(k):
        at = chunk_of(step_of(k, z))
        fwd_copy(k).wait_recv()
        xs[slots:, at] = recv_b[:, :, :, at].astype(F32).reshape(slots, wide_n).astype(BF16)
        if k == 0:
            local[1].wait()
            local[2].wait()
        for a, b in ((0, cut), (cut, half)):
            gt = dot_nt(wg[a:b, at], xs[:, at])
            up = dot_nt(wu[a:b, at], xs[:, at])
            if k > 0:
                gt = gt + gt_ref[a:b]
                up = up + up_ref[a:b]
            if k < line - 1:
                gt_ref[a:b] = gt
                up_ref[a:b] = up
            else:
                hid[:, a:b] = (gt / (1.0 + jnp.exp(-gt)) * up).T.astype(BF16)

    per = LANES // RANK
    near = line * rows
    lane_g = lax.broadcasted_iota(jnp.int32, (group, LANES), 1)
    own = jnp.zeros((group, LANES), jnp.int32)
    for par in range(2):
        ids = []
        for p in range(plane):
            lane = lax.broadcasted_iota(jnp.int32, (near, aid_ref.shape[1]), 1)
            row = lax.broadcasted_iota(jnp.int32, (near, aid_ref.shape[1]), 0)
            here = ((lax.div(row, rows) * plane + p) * 2 + par) * rows + lax.rem(row, rows)
            ids.append(jnp.sum(jnp.where(lane == here, aid_ref[...].astype(F32), 0.0), axis=1, keepdims=True))
        ids = jnp.broadcast_to(jnp.concatenate(ids, axis=0), (group, LANES)).astype(jnp.int32)
        id_hi = lax.div(ids, per)
        tag_ref[par] = id_hi.astype(F32).astype(BF16)
        keep_ref[par] = jnp.where(lax.div(lane_g, RANK) == ids - id_hi * per, 1.0, 0.0)
        own = jnp.where(c == par, id_hi, own)
    tag_t[...] = own.astype(F32).T.astype(BF16)
    relay(0)
    for k in range(1, line):
        relay(k)
    blocks = bank // LANES

    def masked(v, t, k):
        return jnp.where(t == jnp.asarray(k, BF16), v, jnp.zeros_like(v))

    fi = lax.broadcasted_iota(jnp.int32, (LANES, LANES), 0)
    fj = lax.broadcasted_iota(jnp.int32, (LANES, LANES), 1)
    fold = jnp.where(lax.rem(fi, RANK) == lax.rem(fj, RANK), 1.0, 0.0).astype(BF16)
    turn = lax.div(lane_g, RANK) == lax.rem(lax.broadcasted_iota(jnp.int32, (group, LANES), 0), per)

    def down(par):
        cols = col[par].reshape(group, LANES)
        tag = tag_ref[par]
        terms = jnp.zeros((group, LANES), F32)
        for k in range(0, blocks, 2):
            wide = jnp.concatenate([masked(cols, tag, k), masked(cols, tag, k + 1)], axis=1)
            tall = jnp.concatenate(
                [adn[:, k * LANES : (k + 1) * LANES], adn[:, (k + 1) * LANES : (k + 2) * LANES]], axis=0
            )
            terms = terms + jnp.dot(wide, tall, preferred_element_type=F32)
        terms = (terms * keep_ref[par]).astype(BF16)
        folded = jnp.where(turn, jnp.dot(terms, fold, preferred_element_type=F32), 0.0)
        lr_send[par] = jnp.sum(folded.reshape(group // per, per, LANES), axis=1).astype(BF16)
        plane_peers(lambda d: lr1_copy(par, d).start())

    local[0].wait()
    adn_copy.wait_recv()

    @pl.when(c == 0)
    def _():
        receive(0)
        for k in range(1, line):
            receive(k)
            multiply(k - 1)
        multiply(line - 1)

    @pl.when(c == 1)
    def _():
        some_col.wait_recv()
        down(1)
        lr1_recv[pl.ds(g, 1)] = lr_send[1].reshape(1, group // per, LANES)
        for k in range(line):
            receive(k)
        all_col.wait_recv()
        down(0)
        lr1_copy(0, g).start()
        for k in range(line):
            multiply(k)

    local[4].wait()

    def down_sib(i):
        at = chunk_of(turn_of(i, z))
        y = jnp.dot(hid[slots:], wd[:, at], preferred_element_type=F32)
        sib_send[i] = y.reshape(plane, line, cap, wide_n).astype(BF16)
        sib_copy(i).start()

    def finish(i):
        at = chunk_of(turn_of(i, z))
        y = jnp.dot(hid[:slots], wd[:, at], preferred_element_type=F32).reshape(plane, line, cap, wide_n)
        sib_copy(i).wait_recv()
        ret_send[i] = (y + sib_recv[i].astype(F32)).astype(BF16)
        ret_recv[i, pl.ds(g, 1)] = ret_send[i, pl.ds(g, 1)]
        plane_peers(lambda d: ret_copy(i, d, g).start())

    for i in range(line):
        down_sib(i)
    @pl.when(c == 1)
    def _():
        some_lr1.wait_recv()

    @pl.when(c == 0)
    def _():
        all_lr1.wait_recv()

    lr2_send[...] = jnp.sum(lr1_recv[...].astype(F32), axis=0).astype(BF16)
    lr2_recv[pl.ds(z, 1)] = lr2_send[...].reshape(1, group // per, LANES)
    line_far(lambda d: lr2_copy(d, z).start())
    for i in range(line):
        finish(i)

    all_lr2.wait_recv()
    local[3].wait()
    aup_copy.wait_recv()
    low = jnp.sum(lr2_recv[...].astype(F32), axis=0).astype(BF16).astype(F32)
    ranks = jnp.broadcast_to(low.reshape(group // per, 1, LANES), (group // per, per, LANES)).reshape(group, LANES)
    ranks = jnp.where(turn, ranks, 0.0).astype(BF16)
    ranks = jnp.dot(ranks, fold, preferred_element_type=F32) * keep_ref[c]
    ranks = ranks.T.astype(BF16)
    tag = tag_t[...]
    corr = jnp.zeros((LANES, group), F32)
    for k in range(0, blocks, 2):
        tall = jnp.concatenate([masked(ranks, tag, k), masked(ranks, tag, k + 1)], axis=0)
        corr = corr + jnp.dot(aup[:, k * LANES : (k + 2) * LANES], tall, preferred_element_type=F32)
    cor_send[...] = corr.T.astype(BF16).reshape(plane, line, rows, LANES)
    cor_recv[pl.ds(g, 1)] = cor_send[pl.ds(g, 1)]
    plane_peers(lambda d: cor_copy(d, g).start())

    share = LANES // (2 * feats)

    def mix(i):
        some_ret(i).wait_recv()
        j = turn_of(i, z)
        if i == line - 1:
            all_cor.wait_recv()
        for s in range(line):
            back = ret_recv[i, :, s].astype(F32).reshape(block, wide_n).astype(BF16)
            both = line_comb[s]
            routed = jnp.dot(both[:, :block], back, preferred_element_type=F32)
            routed = routed + jnp.dot(both[:, half_l : half_l + block], back, preferred_element_type=F32)
            if i == line - 1:
                delta = []
                for b in range(wide_n // LANES):
                    one = cor_recv[b * share, s].astype(F32)
                    for t in range(1, share):
                        one = one + cor_recv[b * share + t, s].astype(F32)
                    delta.append(one)
                routed = routed + jnp.concatenate(delta, axis=1)
            part_send[i, s] = routed.astype(BF16)
        own_part[pl.ds(j, 1)] = part_send[i, pl.ds(z, 1)].astype(F32)
        line_far(lambda d: part_copy(i, d, z, j).start())

    for i in range(line):
        mix(i)

    for cp in (all_x, all_comb, all_disp, all_lr2, all_cor, all_ret):
        cp.wait_send()

    @pl.when(c == 1)
    def _():
        some_col.wait_send()
        some_lr1.wait_send()
        all_lr1.wait_send()

    @pl.when(c == 0)
    def _():
        all_col.wait_send()

    adn_copy.wait_send()
    aup_copy.wait_send()
    for i in range(line):
        sib_copy(i).wait_send()
        fwd_copy(i).wait_send()
    all_part.wait_recv()
    for j in range(line):
        def add(s, acc):
            return acc + part_recv[far(s), j].astype(F32)

        out_ref[:, j * wide_n : (j + 1) * wide_n] = lax.fori_loop(0, line - 1, add, own_part[j]).astype(BF16)

    all_part.wait_send()


def per_device(tokens, idx, gates, aid, wg, wu, wd, adn, aup):
    devices = lax.axis_size("exp")
    chips = devices // 2
    plane = 1
    while plane * plane < chips:
        plane *= 2
    line = chips // plane
    rows, width = tokens.shape
    top = idx.shape[1]
    half = wd.shape[1]
    feats, bank = adn.shape
    need = 2 * (rows * top // devices + 1)
    cap = -(-need // 8) * 8
    slots = chips * cap
    group = chips * rows
    short = chips * rows * RANK // LANES
    wide_n = width // line
    blocks = lambda *s: pltpu.VMEM(s, BF16)
    full = lambda *s: pltpu.VMEM(s, F32)
    sems = lambda n: pltpu.SemaphoreType.DMA((n,))
    hbm = pl.BlockSpec(memory_space=pl.ANY)
    return pl.pallas_call(
        functools.partial(kernel, line, plane, cap, top),
        out_shape=pltpu.VMEM((rows, width), BF16),
        in_specs=[hbm] * 9,
        out_specs=pl.BlockSpec(memory_space=pltpu.VMEM),
        scratch_shapes=[
            pltpu.VMEM((top, rows), jnp.int32), full(top, rows), pltpu.VMEM((1, aid.shape[0]), jnp.int32),
            blocks(half, width), blocks(half, width), blocks(half, width),
            blocks(LANES, bank), blocks(LANES, bank),
            blocks(line, rows, width), blocks(line, rows, LANES), blocks(line, rows, LANES),
            blocks(line, plane * cap, rows),
            blocks(2, plane, line, rows, LANES),
            blocks(plane, line, cap, width), blocks(plane, line, cap, width), blocks(plane, line, cap, width),
            blocks(2 * slots, width), full(half, 2 * slots), full(half, 2 * slots), blocks(2 * slots, half),
            blocks(line, plane, line, cap, wide_n), blocks(line, plane, line, cap, wide_n),
            blocks(2, group, LANES), blocks(LANES, group), full(2, group, LANES),
            blocks(2, short, LANES), blocks(plane, short, LANES), blocks(short, LANES), blocks(line, short, LANES),
            blocks(plane, line, rows, LANES), blocks(plane, line, rows, LANES),
            blocks(line, plane, line, cap, wide_n), blocks(line, plane, line, cap, wide_n),
            blocks(line, line, rows, wide_n), blocks(line, line, rows, wide_n), full(line, rows, wide_n),
            sems(4), sems(3), sems(2), sems(2), sems(2),
            sems(1), sems(line * line), sems(1), sems(line), sems(1), sems(2), sems(1), sems(line), sems(line), sems(line),
            sems(2), sems(1), sems(1), sems(1), sems(1), sems(1), sems(1), sems(line), sems(1), sems(1),
            sems(line), sems(line),
        ],
        compiler_params=pltpu.CompilerParams(
            collective_id=0, has_side_effects=True, vmem_limit_bytes=62 * 1024 * 1024
        ),
    )(tokens, idx.T, gates.T, aid.reshape(1, -1), wg.swapaxes(1, 2), wu.swapaxes(1, 2), wd, adn, aup)


def solution(mesh):
    placed = (
        P(("grp", "exp"), None),
        P(("grp", "exp"), None),
        P(("grp", "exp"), None),
        P("grp"),
        P("exp", None, None),
        P("exp", None, None),
        P("exp", None, None),
        P("exp", None),
        P("exp", None),
    )
    return jax.shard_map(
        per_device, mesh=mesh, in_specs=placed, out_specs=P(("grp", "exp"), None), check_vma=False
    )
```

```python
import functools

import jax
import jax.numpy as jnp
from jax import lax
from jax.experimental import pallas as pl
from jax.experimental.pallas import tpu as pltpu
from jax.sharding import PartitionSpec as P

RANK = 16
LANES = 128
BF16 = jnp.bfloat16
F32 = jnp.float32
MESH = pl.DeviceIdType.MESH


def dot_nt(a, b):
    return lax.dot_general(a, b, (((1,), (1,)), ((), ())), preferred_element_type=F32)


def kernel(
    line, plane, cap, top, x_hbm, idx_hbm, gate_hbm, aid_hbm, wg_hbm, wu_hbm, wd_hbm, adn_hbm, aup_hbm, out_ref,
    idx_ref, gate_ref, aid_ref, wg, wu, wd, adn, aup, line_x, comb_send, line_comb, pick_ref, col, disp, recv_a,
    recv_b, xs, gt_ref, up_ref, hid, sib_send, sib_recv, tag_ref, tag_t, keep_ref, lr_send, lr1_recv, lr2_send,
    lr2_recv, cor_send, cor_recv, ret_send, ret_recv, part_send, part_recv, own_part, in_sem, w_sem, adl_sem, ad_s,
    ad_r, x_s, x_r, cb_s, cb_r, col_s, col_r, disp_s, disp_r, fwd_s, fwd_r, l1_s, l1_r, l2_s, l2_r, cor_s, cor_r,
    ret_s, ret_r, part_s, part_r, sib_s, sib_r,
):
    me = lax.axis_index("exp")
    q = lax.div(me, 2)
    c = lax.rem(me, 2)
    z = lax.div(q, plane)
    g = lax.rem(q, plane)
    sib = me + 1 - 2 * c
    rows, width = x_hbm.shape
    feats = adn_hbm.shape[0]
    bank = adn_hbm.shape[1]
    chips = line * plane
    group = chips * rows
    slots = chips * cap
    block = plane * cap
    wide_n = width // line
    off = pl.multiple_of(lax.rem(me * feats, LANES), feats)
    half_l = LANES // 2

    def remote(src, dst, ss, rs, dev):
        return pltpu.make_async_remote_copy(
            src_ref=src, dst_ref=dst, send_sem=ss, recv_sem=rs, device_id={"exp": dev}, device_id_type=MESH
        )

    def dev_z(to):
        return 2 * (to * plane + g) + c

    def dev_g(to):
        return 2 * (z * plane + to) + c

    def dev_cross(to):
        return 2 * (z * plane + to) + 1 - c

    side = lax.div(2 * z, line)
    mirror = side * z + (1 - side) * (line - 1 - z)

    def far(s):
        d = s + lax.div(s - mirror + line, line)
        return side * d + (1 - side) * (line - 1 - d)

    def loop(n, fn):
        def step(r, carry):
            fn(r)
            return carry

        lax.fori_loop(0, n, step, 0)

    def line_far(fn):
        loop(line - 1, lambda s: fn(far(s)))

    def line_near(fn):
        loop(line - 1, lambda s: fn(far(line - 2 - s)))

    def plane_peers(fn):
        loop(plane - 1, lambda r: fn(lax.rem(g + 1 + r, plane)))

    barrier = pltpu.get_barrier_semaphore()
    if 2 * feats < LANES:
        adn[...] = jnp.zeros_like(adn)
        aup[...] = jnp.zeros_like(aup)

    def greet(dev):
        pl.semaphore_signal(barrier, inc=1, device_id={"exp": dev}, device_id_type=MESH)

    line_far(lambda d: greet(dev_z(d)))
    plane_peers(lambda d: greet(dev_g(d)))
    plane_peers(lambda d: greet(dev_cross(d)))
    greet(sib)

    own_rows = pl.ds(off, feats)
    inputs = [
        pltpu.make_async_copy(idx_hbm, idx_ref, in_sem.at[0]),
        pltpu.make_async_copy(gate_hbm, gate_ref, in_sem.at[1]),
        pltpu.make_async_copy(x_hbm, line_x.at[z], in_sem.at[2]),
        pltpu.make_async_copy(aid_hbm, aid_ref, in_sem.at[3]),
    ]
    for cp in inputs:
        cp.start()
    local = [
        pltpu.make_async_copy(adn_hbm, adn.at[own_rows], adl_sem.at[0]),
        pltpu.make_async_copy(wg_hbm.at[0], wg, w_sem.at[0]),
        pltpu.make_async_copy(wu_hbm.at[0], wu, w_sem.at[1]),
        pltpu.make_async_copy(aup_hbm, aup.at[own_rows], adl_sem.at[1]),
        pltpu.make_async_copy(wd_hbm.at[0], wd, w_sem.at[2]),
    ]
    for cp in inputs:
        cp.wait()
    for cp in local:
        cp.start()
    pl.semaphore_wait(barrier, line + 2 * plane - 2)

    def step_of(k, at):
        return at if k == 0 else k - 1 + lax.div(k - 1 + line - at, line)

    def lanes_of(chip):
        return pl.ds(pl.multiple_of(lax.div(chip * 2 * feats, LANES) * LANES, LANES), LANES)

    def chunk_of(i):
        return pl.ds(pl.multiple_of(i * wide_n, wide_n), wide_n)

    def x_copy(to, slot, i, kind):
        at = chunk_of(i)
        return remote(line_x.at[z, :, at], line_x.at[slot, :, at], x_s.at[0], x_r.at[kind * line + slot], dev_z(to))

    def comb_copy(to, slot):
        return remote(comb_send.at[to], line_comb.at[slot], cb_s.at[0], cb_r.at[slot], dev_z(to))

    def col_copy(to, s):
        return remote(
            line_x.at[s, :, lanes_of(z * plane + to)], col.at[c, g, s],
            col_s.at[0], col_r.at[c], 2 * (z * plane + to) + 1,
        )

    def disp_copy(to, slot, s, k):
        at = chunk_of(step_of(k, z))
        return remote(disp.at[to, s, :, at], recv_a.at[slot, s, :, at], disp_s.at[0], disp_r.at[k], dev_g(to))

    def fwd_copy(k):
        at = chunk_of(step_of(k, z))
        return remote(recv_a.at[:, :, :, at], recv_b.at[:, :, :, at], fwd_s.at[k], fwd_r.at[k], sib)

    def lr1_copy(par, to):
        return remote(
            lr_send.at[par], lr1_recv.at[g], l1_s.at[par], l1_r.at[0], 2 * (z * plane + to) + par
        )

    def lr2_copy(to, slot):
        return remote(lr2_send, lr2_recv.at[slot], l2_s.at[0], l2_r.at[0], dev_z(to))

    def cor_copy(to, slot):
        return remote(cor_send.at[to], cor_recv.at[slot], cor_s.at[0], cor_r.at[0], dev_g(to))

    def ret_copy(i, to, slot):
        return remote(ret_send.at[i, to], ret_recv.at[i, slot], ret_s.at[0], ret_r.at[i], dev_g(to))

    def turn_of(i, at):
        return lax.rem(at + 1 + i, line)

    def part_copy(i, to, slot, j):
        return remote(part_send.at[i, to], part_recv.at[slot, j], part_s.at[0], part_r.at[0], dev_z(to))

    def sib_copy(i):
        return remote(sib_send.at[i], sib_recv.at[i], sib_s.at[i], sib_r.at[i], sib)

    rest_z = pl.ds(0, line - 1)
    rest_g = pl.ds(0, plane - 1)
    all_x = remote(line_x.at[rest_z], line_x.at[rest_z], x_s.at[0], x_r.at[0], sib)
    all_comb = remote(comb_send.at[rest_z], line_comb.at[rest_z], cb_s.at[0], cb_r.at[0], sib)
    some_col = remote(col.at[1, rest_g], col.at[1, rest_g], col_s.at[0], col_r.at[1], sib)
    all_col = remote(col.at[0], col.at[0], col_s.at[0], col_r.at[0], sib)
    all_disp = remote(disp.at[rest_g], recv_a.at[rest_g], disp_s.at[0], disp_r.at[0], sib)
    some_lr1 = remote(lr1_recv.at[rest_g], lr1_recv.at[rest_g], l1_s.at[1], l1_r.at[0], sib)
    all_lr1 = remote(lr1_recv, lr1_recv, l1_s.at[0], l1_r.at[0], sib)
    all_lr2 = remote(lr2_recv.at[rest_z], lr2_recv.at[rest_z], l2_s.at[0], l2_r.at[0], sib)
    all_cor = remote(cor_send.at[rest_g], cor_recv.at[rest_g], cor_s.at[0], cor_r.at[0], sib)
    all_ret = remote(ret_send.at[:, rest_g], ret_recv.at[:, rest_g], ret_s.at[0], ret_r.at[0], sib)
    all_part = remote(part_send.at[:, rest_z], part_recv.at[rest_z], part_s.at[0], part_r.at[0], sib)

    def some_x(s, k):
        at = chunk_of(0)
        return remote(line_x.at[s, :, at], line_x.at[s, :, at], x_s.at[0], x_r.at[k * line + s], sib)

    def some_disp(k):
        at = chunk_of(0)
        return remote(disp.at[rest_g, :, :, at], recv_a.at[rest_g, :, :, at], disp_s.at[0], disp_r.at[k], sib)

    def some_ret(i):
        return remote(ret_send.at[i, rest_g], ret_recv.at[i, rest_g], ret_s.at[0], ret_r.at[i], sib)

    line_far(lambda d: x_copy(d, z, step_of(0, d), 0).start())
    plane_peers(lambda d: col_copy(d, z).start())
    slot = lax.broadcasted_iota(jnp.int32, (slots, rows), 0)
    slot_e = lax.div(slot, cap)
    chosen = jnp.zeros((slots, rows), F32)
    weight = jnp.zeros((slots, rows), F32)
    for k in range(top):
        hit = idx_ref[k : k + 1, :] == slot_e
        chosen = chosen + jnp.where(hit, 1.0, 0.0)
        weight = weight + jnp.where(hit, gate_ref[k : k + 1, :], 0.0)
    earlier = jnp.where(
        lax.broadcasted_iota(jnp.int32, (rows, rows), 0) < lax.broadcasted_iota(jnp.int32, (rows, rows), 1), 1.0, 0.0
    )
    rank_of = jnp.dot(chosen.astype(BF16), earlier.astype(BF16), preferred_element_type=F32)
    slot_p = lax.rem(slot, cap).astype(F32)
    combine = jnp.where((chosen > 0.5) & (rank_of == slot_p), weight, 0.0)
    for d in range(line):
        part = combine[d * block : (d + 1) * block].T
        hi = part.astype(BF16)
        lo = (part - hi.astype(F32)).astype(BF16)
        comb_send[d, :, :block] = hi
        comb_send[d, :, half_l : half_l + block] = lo
    line_comb[pl.ds(z, 1)] = comb_send[pl.ds(z, 1)]

    line_far(lambda d: comb_copy(d, z).start())
    for k in range(1, line):
        line_far(lambda d: x_copy(d, z, step_of(k, d), k).start())
    adn_copy = remote(adn_hbm, adn.at[own_rows], ad_s.at[0], ad_r.at[0], sib)
    aup_copy = remote(aup_hbm, aup.at[own_rows], ad_s.at[1], ad_r.at[1], sib)
    adn_copy.start()
    aup_copy.start()

    def own_col(s):
        @pl.when(c == 1)
        def _():
            col[1, pl.ds(g, 1), pl.ds(s, 1)] = line_x[pl.ds(s, 1), :, lanes_of(q)].reshape(1, 1, rows, LANES)

        @pl.when(c == 0)
        def _():
            col_copy(g, s).start()

    def take_pick(s):
        pick = jnp.where(line_comb[s].astype(F32) != 0.0, 1.0, 0.0).T[:block]
        pick_ref[pl.ds(s, 1)] = pick.astype(BF16).reshape(1, block, rows)

    def pack(s, k):
        at = chunk_of(step_of(k, z))
        packed = jnp.dot(pick_ref[s], line_x[s, :, at], preferred_element_type=F32)
        disp[:, pl.ds(s, 1), :, at] = packed.reshape(plane, 1, cap, wide_n).astype(BF16)
        recv_a[pl.ds(g, 1), pl.ds(s, 1), :, at] = disp[pl.ds(g, 1), pl.ds(s, 1), :, at]
        plane_peers(lambda d: disp_copy(d, g, s, k).start())

    take_pick(z)
    for k in range(line):
        pack(z, k)
    own_col(z)

    near_z = [far(line - 2 - k) for k in range(line - 1)]
    half = wd.shape[0]
    cut = -(-half // (2 * LANES)) * LANES

    def relay(k):
        for s in near_z:
            some_x(s, k).wait_recv()
            if k == 0:
                plane_peers(lambda d: col_copy(d, s).start())
                own_col(s)
                comb_copy(z, s).wait_recv()
                take_pick(s)
            pack(s, k)

    def receive(k):
        at = chunk_of(step_of(k, z))
        some_disp(k).wait_recv()
        fwd_copy(k).start()
        xs[:slots, at] = recv_a[:, :, :, at].astype(F32).reshape(slots, wide_n).astype(BF16)

    def multiply(k):
        at = chunk_of(step_of(k, z))
        fwd_copy(k).wait_recv()
        xs[slots:, at] = recv_b[:, :, :, at].astype(F32).reshape(slots, wide_n).astype(BF16)
        if k == 0:
            local[1].wait()
            local[2].wait()
        for a, b in ((0, cut), (cut, half)):
            gt = dot_nt(wg[a:b, at], xs[:, at])
            up = dot_nt(wu[a:b, at], xs[:, at])
            if k > 0:
                gt = gt + gt_ref[a:b]
                up = up + up_ref[a:b]
            if k < line - 1:
                gt_ref[a:b] = gt
                up_ref[a:b] = up
            else:
                hid[:, a:b] = (gt / (1.0 + jnp.exp(-gt)) * up).T.astype(BF16)

    per = LANES // RANK
    near = line * rows
    lane_g = lax.broadcasted_iota(jnp.int32, (group, LANES), 1)
    own = jnp.zeros((group, LANES), jnp.int32)
    for par in range(2):
        ids = []
        for p in range(plane):
            lane = lax.broadcasted_iota(jnp.int32, (near, aid_ref.shape[1]), 1)
            row = lax.broadcasted_iota(jnp.int32, (near, aid_ref.shape[1]), 0)
            here = ((lax.div(row, rows) * plane + p) * 2 + par) * rows + lax.rem(row, rows)
            ids.append(jnp.sum(jnp.where(lane == here, aid_ref[...].astype(F32), 0.0), axis=1, keepdims=True))
        ids = jnp.broadcast_to(jnp.concatenate(ids, axis=0), (group, LANES)).astype(jnp.int32)
        id_hi = lax.div(ids, per)
        tag_ref[par] = id_hi.astype(F32).astype(BF16)
        keep_ref[par] = jnp.where(lax.div(lane_g, RANK) == ids - id_hi * per, 1.0, 0.0)
        own = jnp.where(c == par, id_hi, own)
    tag_t[...] = own.astype(F32).T.astype(BF16)
    relay(0)
    for k in range(1, line):
        relay(k)
    blocks = bank // LANES

    def masked(v, t, k):
        return jnp.where(t == jnp.asarray(k, BF16), v, jnp.zeros_like(v))

    def fold_turn():
        fi = lax.broadcasted_iota(jnp.int32, (LANES, LANES), 0)
        fj = lax.broadcasted_iota(jnp.int32, (LANES, LANES), 1)
        fold = jnp.where(lax.rem(fi, RANK) == lax.rem(fj, RANK), 1.0, 0.0).astype(BF16)
        lane = lax.broadcasted_iota(jnp.int32, (group, LANES), 1)
        row = lax.broadcasted_iota(jnp.int32, (group, LANES), 0)
        return fold, lax.div(lane, RANK) == lax.rem(row, per)


    def down(par):
        cols = col[par].reshape(group, LANES)
        tag = tag_ref[par]
        terms = jnp.zeros((group, LANES), F32)
        for k in range(0, blocks, 2):
            wide = jnp.concatenate([masked(cols, tag, k), masked(cols, tag, k + 1)], axis=1)
            tall = jnp.concatenate(
                [adn[:, k * LANES : (k + 1) * LANES], adn[:, (k + 1) * LANES : (k + 2) * LANES]], axis=0
            )
            terms = terms + jnp.dot(wide, tall, preferred_element_type=F32)
        fold, turn = fold_turn()
        terms = (terms * keep_ref[par]).astype(BF16)
        folded = jnp.where(turn, jnp.dot(terms, fold, preferred_element_type=F32), 0.0)
        lr_send[par] = jnp.sum(folded.reshape(group // per, per, LANES), axis=1).astype(BF16)
        plane_peers(lambda d: lr1_copy(par, d).start())

    local[0].wait()
    adn_copy.wait_recv()

    @pl.when(c == 0)
    def _():
        receive(0)
        for k in range(1, line):
            receive(k)
            multiply(k - 1)
        multiply(line - 1)

    @pl.when(c == 1)
    def _():
        some_col.wait_recv()
        down(1)
        lr1_recv[pl.ds(g, 1)] = lr_send[1].reshape(1, group // per, LANES)
        for k in range(line):
            receive(k)
        all_col.wait_recv()
        down(0)
        lr1_copy(0, g).start()
        for k in range(line):
            multiply(k)

    local[4].wait()

    def down_sib(i):
        at = chunk_of(turn_of(i, z))
        y = jnp.dot(hid[slots:], wd[:, at], preferred_element_type=F32)
        sib_send[i] = y.reshape(plane, line, cap, wide_n).astype(BF16)
        sib_copy(i).start()

    def finish(i):
        at = chunk_of(turn_of(i, z))
        y = jnp.dot(hid[:slots], wd[:, at], preferred_element_type=F32).reshape(plane, line, cap, wide_n)
        sib_copy(i).wait_recv()
        ret_send[i] = (y + sib_recv[i].astype(F32)).astype(BF16)
        ret_recv[i, pl.ds(g, 1)] = ret_send[i, pl.ds(g, 1)]
        plane_peers(lambda d: ret_copy(i, d, g).start())

    def low_sum():
        lr2_send[...] = jnp.sum(lr1_recv[...].astype(F32), axis=0).astype(BF16)
        lr2_recv[pl.ds(z, 1)] = lr2_send[...].reshape(1, group // per, LANES)
        line_far(lambda d: lr2_copy(d, z).start())

    @pl.when(c == 0)
    def _():
        for i in range(line):
            down_sib(i)
        all_lr1.wait_recv()
        low_sum()
        for i in range(line):
            finish(i)

    @pl.when(c == 1)
    def _():
        down_sib(0)
        finish(0)
        down_sib(1)
        some_lr1.wait_recv()
        low_sum()
        finish(1)
        for i in range(2, line):
            down_sib(i)
        for i in range(2, line):
            finish(i)

    all_lr2.wait_recv()
    local[3].wait()
    aup_copy.wait_recv()
    fold, turn = fold_turn()
    low = jnp.sum(lr2_recv[...].astype(F32), axis=0).astype(BF16).astype(F32)
    ranks = jnp.broadcast_to(low.reshape(group // per, 1, LANES), (group // per, per, LANES)).reshape(group, LANES)
    ranks = jnp.where(turn, ranks, 0.0).astype(BF16)
    ranks = jnp.dot(ranks, fold, preferred_element_type=F32) * keep_ref[c]
    ranks = ranks.T.astype(BF16)
    tag = tag_t[...]
    corr = jnp.zeros((LANES, group), F32)
    for k in range(0, blocks, 2):
        tall = jnp.concatenate([masked(ranks, tag, k), masked(ranks, tag, k + 1)], axis=0)
        corr = corr + jnp.dot(aup[:, k * LANES : (k + 2) * LANES], tall, preferred_element_type=F32)
    cor_send[...] = corr.T.astype(BF16).reshape(plane, line, rows, LANES)
    cor_recv[pl.ds(g, 1)] = cor_send[pl.ds(g, 1)]
    plane_peers(lambda d: cor_copy(d, g).start())

    share = LANES // (2 * feats)

    def mix(i):
        some_ret(i).wait_recv()
        j = turn_of(i, z)
        if i == line - 1:
            all_cor.wait_recv()
        for s in range(line):
            back = ret_recv[i, :, s].astype(F32).reshape(block, wide_n).astype(BF16)
            both = line_comb[s]
            routed = jnp.dot(both[:, :block], back, preferred_element_type=F32)
            routed = routed + jnp.dot(both[:, half_l : half_l + block], back, preferred_element_type=F32)
            if i == line - 1:
                delta = []
                for b in range(wide_n // LANES):
                    one = cor_recv[b * share, s].astype(F32)
                    for t in range(1, share):
                        one = one + cor_recv[b * share + t, s].astype(F32)
                    delta.append(one)
                routed = routed + jnp.concatenate(delta, axis=1)
            part_send[i, s] = routed.astype(BF16)
        own_part[pl.ds(j, 1)] = part_send[i, pl.ds(z, 1)].astype(F32)
        line_far(lambda d: part_copy(i, d, z, j).start())

    for i in range(line):
        mix(i)

    for cp in (all_x, all_comb, all_disp, all_lr2, all_cor, all_ret):
        cp.wait_send()

    @pl.when(c == 1)
    def _():
        some_col.wait_send()
        some_lr1.wait_send()
        all_lr1.wait_send()

    @pl.when(c == 0)
    def _():
        all_col.wait_send()

    adn_copy.wait_send()
    aup_copy.wait_send()
    for i in range(line):
        sib_copy(i).wait_send()
        fwd_copy(i).wait_send()
    all_part.wait_recv()
    for j in range(line):
        def add(s, acc):
            return acc + part_recv[far(s), j].astype(F32)

        out_ref[:, j * wide_n : (j + 1) * wide_n] = lax.fori_loop(0, line - 1, add, own_part[j]).astype(BF16)

    all_part.wait_send()


def per_device(tokens, idx, gates, aid, wg, wu, wd, adn, aup):
    devices = lax.axis_size("exp")
    chips = devices // 2
    plane = 1
    while plane * plane < chips:
        plane *= 2
    line = chips // plane
    rows, width = tokens.shape
    top = idx.shape[1]
    half = wd.shape[1]
    feats, bank = adn.shape
    need = 2 * (rows * top // devices + 1)
    cap = -(-need // 8) * 8
    slots = chips * cap
    group = chips * rows
    short = chips * rows * RANK // LANES
    wide_n = width // line
    blocks = lambda *s: pltpu.VMEM(s, BF16)
    full = lambda *s: pltpu.VMEM(s, F32)
    sems = lambda n: pltpu.SemaphoreType.DMA((n,))
    hbm = pl.BlockSpec(memory_space=pl.ANY)
    return pl.pallas_call(
        functools.partial(kernel, line, plane, cap, top),
        out_shape=pltpu.VMEM((rows, width), BF16),
        in_specs=[hbm] * 9,
        out_specs=pl.BlockSpec(memory_space=pltpu.VMEM),
        scratch_shapes=[
            pltpu.VMEM((top, rows), jnp.int32), full(top, rows), pltpu.VMEM((1, aid.shape[0]), jnp.int32),
            blocks(half, width), blocks(half, width), blocks(half, width),
            blocks(LANES, bank), blocks(LANES, bank),
            blocks(line, rows, width), blocks(line, rows, LANES), blocks(line, rows, LANES),
            blocks(line, plane * cap, rows),
            blocks(2, plane, line, rows, LANES),
            blocks(plane, line, cap, width), blocks(plane, line, cap, width), blocks(plane, line, cap, width),
            blocks(2 * slots, width), full(half, 2 * slots), full(half, 2 * slots), blocks(2 * slots, half),
            blocks(line, plane, line, cap, wide_n), blocks(line, plane, line, cap, wide_n),
            blocks(2, group, LANES), blocks(LANES, group), full(2, group, LANES),
            blocks(2, short, LANES), blocks(plane, short, LANES), blocks(short, LANES), blocks(line, short, LANES),
            blocks(plane, line, rows, LANES), blocks(plane, line, rows, LANES),
            blocks(line, plane, line, cap, wide_n), blocks(line, plane, line, cap, wide_n),
            blocks(line, line, rows, wide_n), blocks(line, line, rows, wide_n), full(line, rows, wide_n),
            sems(4), sems(3), sems(2), sems(2), sems(2),
            sems(1), sems(line * line), sems(1), sems(line), sems(1), sems(2), sems(1), sems(line), sems(line), sems(line),
            sems(2), sems(1), sems(1), sems(1), sems(1), sems(1), sems(1), sems(line), sems(1), sems(1),
            sems(line), sems(line),
        ],
        compiler_params=pltpu.CompilerParams(
            collective_id=0, has_side_effects=True, vmem_limit_bytes=62 * 1024 * 1024
        ),
    )(tokens, idx.T, gates.T, aid.reshape(1, -1), wg.swapaxes(1, 2), wu.swapaxes(1, 2), wd, adn, aup)


def solution(mesh):
    placed = (
        P(("grp", "exp"), None),
        P(("grp", "exp"), None),
        P(("grp", "exp"), None),
        P("grp"),
        P("exp", None, None),
        P("exp", None, None),
        P("exp", None, None),
        P("exp", None),
        P("exp", None),
    )
    return jax.shard_map(
        per_device, mesh=mesh, in_specs=placed, out_specs=P(("grp", "exp"), None), check_vma=False
    )
```
